16 devices in a mesh: rep: 2 (over y, z), stage: 8 (over x, core).
Axes of the slice: x: 4, y: 2, z: 1, core: 2. Of those that a mesh axis runs over, the one named last changes fastest.
The devices are a block of a 4x4x8 slice.
Arguments:
- embeds: bfloat16 [16, 2, 256, 1024], P('rep'), parts along dimension 0
- targets: bfloat16 [16, 2, 256, 1024], P('rep'), parts along dimension 0
- w_qkv: bfloat16 [8, 1024, 3072], P('stage')
- w_out: bfloat16 [8, 16, 64, 1024], P('stage')
- w_up: bfloat16 [8, 1024, 4096], P('stage')
- w_down: bfloat16 [8, 4096, 1024], P('stage')
Outputs:
- output 1: float32 [2], P('rep'), parts along dimension 0
- output 2: float32 [16, 1024, 3072], P(('rep', 'stage')), parts along dimension 0
- output 3: float32 [16, 16, 64, 1024], P(('rep', 'stage')), parts along dimension 0
- output 4: float32 [16, 1024, 4096], P(('rep', 'stage')), parts along dimension 0
- output 5: float32 [16, 4096, 1024], P(('rep', 'stage')), parts along dimension 0
- output 6: bfloat16 [16, 2, 256, 1024], P('rep'), parts along dimension 0
There are 2 independent parts. The reference program is written for one: setup_inputs(seed, part) draws one part's arguments, and reference() takes and returns one part's arrays. A program takes and returns all parts, laid end to end along the dimension named above; an argument that names none is the same for every part.
All inputs are finite; a program needn't handle non-finite values.
Results may differ from the reference program's by a relative error of at most 0.02.
Values are sent between devices in bfloat16 or wider.
A program may use at most 768 MiB of HBM per device.

```python
import jax
import jax.numpy as jnp
from jax import lax

MODEL_DIM = 1024
NUM_HEADS = 16
NUM_STAGES = 8
NUM_MICRO = 8
MICRO_BATCH = 2
SEQ_LEN = 256
NORM_EPS = 1e-6
NEG_BIG = -1e30


def setup_inputs(seed: int = 0, part: int = 0) -> dict:
    root_key = jax.random.key(seed)
    key_qkv, key_out, key_up, key_down, key_data = jax.random.split(root_key, 5)
    key_emb, key_tgt = jax.random.split(jax.random.fold_in(key_data, part), 2)
    head_dim = MODEL_DIM // NUM_HEADS
    ff_dim = 4 * MODEL_DIM
    act_shape = (NUM_MICRO, MICRO_BATCH, SEQ_LEN, MODEL_DIM)
    embeds = jax.random.normal(key_emb, act_shape, jnp.float32)
    targets = jax.random.normal(key_tgt, act_shape, jnp.float32)
    w_qkv = jax.random.normal(key_qkv, (NUM_STAGES, MODEL_DIM, 3 * MODEL_DIM), jnp.float32) * MODEL_DIM ** -0.5
    w_out = jax.random.normal(key_out, (NUM_STAGES, NUM_HEADS, head_dim, MODEL_DIM), jnp.float32) * MODEL_DIM ** -0.5
    w_up = jax.random.normal(key_up, (NUM_STAGES, MODEL_DIM, ff_dim), jnp.float32) * MODEL_DIM ** -0.5
    w_down = jax.random.normal(key_down, (NUM_STAGES, ff_dim, MODEL_DIM), jnp.float32) * ff_dim ** -0.5
    return {'embeds': embeds.astype(jnp.bfloat16), 'targets': targets.astype(jnp.bfloat16), 'w_qkv': w_qkv.astype(jnp.bfloat16), 'w_out': w_out.astype(jnp.bfloat16), 'w_up': w_up.astype(jnp.bfloat16), 'w_down': w_down.astype(jnp.bfloat16)}


def rms_norm(vals):
    return vals * lax.rsqrt(jnp.mean(vals * vals, axis=-1, keepdims=True) + NORM_EPS)


def layer_forward(act_in, w_qkv, w_out, w_up, w_down):
    batch_size, seq_len = act_in.shape[0], act_in.shape[1]
    num_heads, head_dim = w_out.shape[0], w_out.shape[1]
    act_f = act_in.astype(jnp.float32)
    normed = rms_norm(act_f).astype(jnp.bfloat16)
    qkv_flat = jnp.dot(normed.astype(jnp.float32), w_qkv).astype(jnp.bfloat16)
    qkv_heads = qkv_flat.reshape(batch_size, seq_len, 3, num_heads, head_dim).astype(jnp.float32)
    scores = (jnp.einsum('bqhd,bkhd->bhqk', qkv_heads[:, :, 0], qkv_heads[:, :, 1]) * head_dim ** -0.5).astype(jnp.bfloat16)
    causal = jnp.arange(seq_len)[:, None] >= jnp.arange(seq_len)[None, :]
    attn_probs = jax.nn.softmax(jnp.where(causal, scores.astype(jnp.float32), NEG_BIG), axis=-1).astype(jnp.bfloat16)
    context = jnp.einsum('bhqk,bkhd->bqhd', attn_probs.astype(jnp.float32), qkv_heads[:, :, 2]).astype(jnp.bfloat16)
    hidden = (act_f + jnp.einsum('bqhd,hde->bqe', context.astype(jnp.float32), w_out)).astype(jnp.bfloat16)
    hidden_f = hidden.astype(jnp.float32)
    normed2 = rms_norm(hidden_f).astype(jnp.bfloat16)
    pre_act = jnp.dot(normed2.astype(jnp.float32), w_up).astype(jnp.bfloat16)
    gelu_out = jax.nn.gelu(pre_act.astype(jnp.float32)).astype(jnp.bfloat16)
    return (hidden_f + jnp.dot(gelu_out.astype(jnp.float32), w_down)).astype(jnp.bfloat16)


def reference(embeds, targets, w_qkv, w_out, w_up, w_down):
    norm_count = NUM_MICRO * MICRO_BATCH * SEQ_LEN * MODEL_DIM
    weights = (w_qkv, w_out, w_up, w_down)

    def fwd_layer(act_in, layer_w):
        wide_w = [w_one.astype(jnp.float32) for w_one in layer_w]
        return layer_forward(act_in, *wide_w), act_in

    def bwd_layer(grad_in, layer_data):
        wide_w = [w_one.astype(jnp.float32) for w_one in layer_data[1:]]
        pullback = jax.vjp(layer_forward, layer_data[0], *wide_w)[1]
        grads_all = pullback(grad_in)
        return grads_all[0], tuple(grads_all[1:])

    def micro_step(grad_acc, micro_data):
        embed_m, target_m = micro_data
        top_out, stored = lax.scan(fwd_layer, embed_m, weights)
        err_vals = top_out.astype(jnp.float32) - target_m.astype(jnp.float32)
        loss_m = 0.5 * jnp.sum(err_vals * err_vals) / norm_count
        seed_grad = (err_vals / norm_count).astype(jnp.bfloat16)
        d_embed, layer_grads = lax.scan(bwd_layer, seed_grad, (stored,) + weights, reverse=True)
        new_acc = tuple(acc_w + grad_w for acc_w, grad_w in zip(grad_acc, layer_grads))
        return new_acc, (d_embed, loss_m)

    zero_grads = tuple(jnp.zeros(w_one.shape, jnp.float32) for w_one in weights)
    grad_sums, (d_embeds, losses) = lax.scan(micro_step, zero_grads, (embeds, targets))
    return (jnp.sum(losses).reshape(1), grad_sums[0], grad_sums[1], grad_sums[2], grad_sums[3], d_embeds)
```

```python
import functools

import jax
import jax.numpy as jnp
from jax import lax
from jax.experimental import pallas as pl
from jax.experimental.pallas import tpu as pltpu
from jax.sharding import PartitionSpec as P

F32, BF16 = jnp.float32, jnp.bfloat16
MESH = pl.DeviceIdType.MESH
NORM_EPS = 1e-6
NEG_BIG = -1e30
GELU_SCALE, GELU_CUBE = 0.7978845608028654, 0.044715


def mm(lhs, rhs):
    return jnp.dot(lhs, rhs, preferred_element_type=F32)


def mm_rt(lhs, rhs):
    return lax.dot_general(lhs, rhs, (((1,), (1,)), ((), ())), preferred_element_type=F32)


def mm_lt(lhs, rhs):
    return lax.dot_general(lhs, rhs, (((0,), (0,)), ((), ())), preferred_element_type=F32)


def inv_rms(vals):
    return lax.rsqrt(jnp.mean(vals * vals, axis=-1, keepdims=True) + NORM_EPS)


def norm_vjp(vals, d_out):
    scale = inv_rms(vals)
    return d_out * scale - vals * (scale * scale * scale * jnp.mean(vals * d_out, axis=-1, keepdims=True))


def gelu(x):
    return (0.5 * x) * (1.0 + jnp.tanh(GELU_SCALE * (x + GELU_CUBE * (x * x * x))))


def gelu_grad(x):
    x_sq = x * x
    t = jnp.tanh(GELU_SCALE * (x + GELU_CUBE * (x_sq * x)))
    return 0.5 * (1.0 + t) + (0.5 * x) * (1.0 - t * t) * (GELU_SCALE * (1.0 + (3 * GELU_CUBE) * x_sq))


def head_half(vals, which):
    lane = lax.broadcasted_iota(jnp.int32, (1, vals.shape[1]), 1)
    half = vals.shape[1] // 2
    return jnp.where((lane < half) if which == 0 else (lane >= half), vals, jnp.zeros_like(vals))


def probs(query, key, causal, scale):
    scores = (mm_rt(query, key) * scale).astype(BF16).astype(F32)
    scores = jnp.where(causal, scores, NEG_BIG)
    top = jnp.max(scores, axis=-1, keepdims=True)
    e = jnp.exp(scores - top)
    return e * (1.0 / jnp.sum(e, axis=-1, keepdims=True))


def attn_fwd(qkv, ctx, rows, width, scale):
    causal = lax.broadcasted_iota(jnp.int32, (rows, rows), 0) >= lax.broadcasted_iota(jnp.int32, (rows, rows), 1)
    for p in range(width // 128):
        q, k, v = (qkv[:, w * width + 128 * p : w * width + 128 * p + 128] for w in range(3))
        a = [probs(head_half(q, h), k, causal, scale).astype(BF16) for h in range(2)]
        both = mm(jnp.concatenate(a, 1), jnp.concatenate([head_half(v, 0), head_half(v, 1)], 0))
        ctx[:, 128 * p : 128 * p + 128] = both.astype(BF16)


def attn_bwd(qkv, d_ctx, d_qkv, rows, width, scale):
    causal = lax.broadcasted_iota(jnp.int32, (rows, rows), 0) >= lax.broadcasted_iota(jnp.int32, (rows, rows), 1)
    for p in range(width // 128):
        q, k, v = (qkv[:, w * width + 128 * p : w * width + 128 * p + 128] for w in range(3))
        d = d_ctx[:, 128 * p : 128 * p + 128]
        a_b, ds_b = [], []
        for h in range(2):
            a = probs(head_half(q, h), k, causal, scale)
            dp = mm_rt(head_half(d, h), v).astype(BF16).astype(F32)
            ds_b.append((a * (dp - jnp.sum(a * dp, axis=-1, keepdims=True))).astype(BF16))
            a_b.append(a.astype(BF16))
        split = lambda vals: jnp.concatenate([head_half(vals, 0), head_half(vals, 1)], 0)
        dq = mm(jnp.concatenate(ds_b, 1), split(k)) * scale
        dk = mm_lt(jnp.concatenate(ds_b, 0), split(q)) * scale
        dv = mm_lt(jnp.concatenate(a_b, 0), split(d))
        for w, val in enumerate((dq, dk, dv)):
            d_qkv[:, w * width + 128 * p : w * width + 128 * p + 128] = val.astype(BF16)


def pipeline_kernel(
    axis, stages, units, scale, inv_count,
    embeds, targets, w_qkv_h, w_out_h, w_up_h, w_down_h,
    xn_all, ctx_all, z_all, gl_all, dqkv_all, dh_all, dpre_all, g_all, dx_all, qkv_all, h_all, pre_all, loss,
    w_qkv, w_out, w_up, w_down, act, grad, out, d_in, target,
    xn, qkv, ctx, hid, z, pre, gl, dpre, dh, dctx, dqkv,
    w_sem, emb_sem, tgt_sem, f_send, f_recv, b_send, b_recv, f_save, b_save, b_load,
):
    stage = lax.axis_index(axis)
    last = stages - 1
    rows, width = act.shape[1], act.shape[2]
    right, left = lax.rem(stage + 1, stages), lax.rem(stage + last, stages)
    barrier = pltpu.get_barrier_semaphore()
    for neighbour in (left, right):
        pl.semaphore_signal(barrier, inc=1, device_id={axis: neighbour}, device_id_type=MESH)

    w_copies = [
        pltpu.make_async_copy(src, dst, w_sem.at[i])
        for i, (src, dst) in enumerate(((w_qkv_h, w_qkv), (w_out_h, w_out), (w_up_h, w_up), (w_down_h, w_down)))
    ]

    def embed_copy(unit):
        return pltpu.make_async_copy(embeds.at[unit], act.at[unit], emb_sem.at[unit])

    @pl.when(stage == 0)
    def _():
        embed_copy(0).start()

    for copy in w_copies:
        copy.start()

    @pl.when(stage == 0)
    def _():
        lax.fori_loop(1, units, lambda unit, c: (embed_copy(unit).start(), c)[1], 0)

    pl.semaphore_wait(barrier, 2)
    loss[...] = jnp.zeros_like(loss)

    def f_copy(unit):
        return pltpu.make_async_remote_copy(
            src_ref=out.at[lax.rem(unit, 2)], dst_ref=act.at[unit], send_sem=f_send.at[lax.rem(unit, 2)],
            recv_sem=f_recv.at[unit], device_id={axis: right}, device_id_type=MESH)

    def b_copy(unit):
        return pltpu.make_async_remote_copy(
            src_ref=d_in.at[lax.rem(unit, 2)], dst_ref=grad.at[unit], send_sem=b_send.at[lax.rem(unit, 2)],
            recv_sem=b_recv.at[unit], device_id={axis: left}, device_id_type=MESH)

    def dx_copy(unit):
        return pltpu.make_async_copy(d_in.at[lax.rem(unit, 2)], dx_all.at[unit], b_send.at[lax.rem(unit, 2)])

    def f_saves(unit):
        pairs = ((xn, xn_all), (qkv.at[0], qkv_all), (ctx, ctx_all), (hid.at[0], h_all), (z, z_all), (pre.at[0], pre_all), (gl, gl_all))
        return [pltpu.make_async_copy(src, dst.at[unit], f_save.at[i]) for i, (src, dst) in enumerate(pairs)]

    def b_saves(unit):
        pairs = ((dpre, dpre_all), (dh, dh_all), (dqkv, dqkv_all), (grad.at[unit], g_all))
        return [pltpu.make_async_copy(src, dst.at[unit], b_save.at[i]) for i, (src, dst) in enumerate(pairs)]

    def b_loads(unit):
        pairs = ((pre_all, pre.at[1]), (h_all, hid.at[1]), (qkv_all, qkv.at[1]))
        return [pltpu.make_async_copy(src.at[unit], dst, b_load.at[i]) for i, (src, dst) in enumerate(pairs)]

    def target_copy(unit):
        return pltpu.make_async_copy(targets.at[unit], target, tgt_sem)

    def forward(unit):
        slot = lax.rem(unit, 2)

        @pl.when(stage == last)
        def _():
            target_copy(unit).start()

        @pl.when(stage == 0)
        def _():
            embed_copy(unit).wait()

        @pl.when(stage > 0)
        def _():
            f_copy(unit).wait_recv()

        @pl.when(unit == 0)
        def _():
            w_copies[0].wait()

        saves = f_saves(unit)
        x = act[unit].astype(F32)
        xn[...] = (x * inv_rms(x)).astype(BF16)
        qkv[0] = mm(xn[...], w_qkv[...]).astype(BF16)
        attn_fwd(qkv.at[0], ctx, rows, width, scale)

        @pl.when(unit == 0)
        def _():
            for copy in w_copies[1:]:
                copy.wait()

        for i in range(3):
            saves[i].start()
        h = (act[unit].astype(F32) + mm(ctx[...], w_out[...])).astype(BF16)
        hid[0] = h
        h = h.astype(F32)
        z[...] = (h * inv_rms(h)).astype(BF16)
        for i in range(3, 5):
            saves[i].start()
        p = mm(z[...], w_up[...]).astype(BF16)
        pre[0] = p
        gl[...] = gelu(p.astype(F32)).astype(BF16)
        for i in range(5, 7):
            saves[i].start()

        @pl.when((stage < last) & (unit >= 2))
        def _():
            f_copy(unit).wait_send()

        out[slot] = (hid[0].astype(F32) + mm(gl[...], w_down[...])).astype(BF16)

        @pl.when(stage < last)
        def _():
            f_copy(unit).start()

        @pl.when(stage == last)
        def _():
            target_copy(unit).wait()
            err = out[slot].astype(F32) - target[...].astype(F32)
            grad[unit] = (err * inv_count).astype(BF16)
            part = jnp.sum((err * err).reshape(rows // 8, 8, width // 128, 128), axis=(0, 2))
            loss[...] += part * (0.5 * inv_count)

    def backward(unit):
        src = jnp.where(stage == last, 0, 1)
        slot = lax.rem(unit, 2)

        @pl.when(stage < last)
        def _():
            b_copy(unit).wait_recv()
            for copy in b_loads(unit):
                copy.wait()

        saves = b_saves(unit)

        @pl.when(unit > 0)
        def _():
            for copy in b_saves(unit - 1):
                copy.wait()

        saves[3].start()
        d_gelu = mm_rt(grad[unit], w_down[...]).astype(BF16).astype(F32)
        dpre[...] = (d_gelu * gelu_grad(pre[src].astype(F32))).astype(BF16)
        saves[0].start()
        dz = mm_rt(dpre[...], w_up[...]).astype(BF16).astype(F32)
        d_hid = (grad[unit].astype(F32) + norm_vjp(hid[src].astype(F32), dz)).astype(BF16)
        dh[...] = d_hid
        saves[1].start()
        dctx[...] = mm_rt(d_hid, w_out[...]).astype(BF16)
        attn_bwd(qkv.at[src], dctx, dqkv, rows, width, scale)
        saves[2].start()

        @pl.when(unit >= 2)
        def _():
            @pl.when(stage > 0)
            def _():
                b_copy(unit).wait_send()

            @pl.when(stage == 0)
            def _():
                dx_copy(unit).wait()

        du = mm_rt(dqkv[...], w_qkv[...]).astype(BF16).astype(F32)
        d_in[slot] = (dh[...].astype(F32) + norm_vjp(act[unit].astype(F32), du)).astype(BF16)

        @pl.when(stage > 0)
        def _():
            b_copy(unit).start()

        @pl.when(stage == 0)
        def _():
            dx_copy(unit).start()

    def tick(t, carry):
        f_unit = t - stage
        b_unit = t - 2 * last + stage

        @pl.when((f_unit >= 1) & (f_unit <= units))
        def _():
            for copy in f_saves(f_unit - 1):
                copy.wait()

        @pl.when((f_unit >= 0) & (f_unit < units))
        def _():
            forward(f_unit)

        @pl.when((b_unit >= 0) & (b_unit < units))
        def _():
            backward(b_unit)

        @pl.when((stage < last) & (b_unit >= -1) & (b_unit < units - 1))
        def _():
            for copy in b_loads(b_unit + 1):
                copy.start()

        return carry

    lax.fori_loop(0, units + 2 * last, tick, 0)

    for copy in b_saves(units - 1):
        copy.wait()

    for unit in (units - 2, units - 1):
        @pl.when(stage < last)
        def _():
            f_copy(unit).wait_send()

        @pl.when(stage > 0)
        def _():
            b_copy(unit).wait_send()

        @pl.when(stage == 0)
        def _():
            dx_copy(unit).wait()


def run_pipeline(axis, stages, embeds, targets, w_qkv, w_out, w_up, w_down, head_dim):
    units, rows, width = embeds.shape
    ff = w_up.shape[1]
    act_t = lambda n: jax.ShapeDtypeStruct((units, rows, n), BF16)
    hbm = pl.BlockSpec(memory_space=pl.ANY)
    row_t = lambda *shape: pltpu.VMEM(shape, BF16)
    dma = pltpu.SemaphoreType.DMA
    outs = [act_t(n) for n in (width, width, width, ff, 3 * width, width, ff, width, width, 3 * width, width, ff)]
    outs.append(jax.ShapeDtypeStruct((8, 128), F32))
    return pl.pallas_call(
        functools.partial(pipeline_kernel, axis, stages, units, head_dim ** -0.5, 1.0 / (units * rows * width)),
        out_shape=outs,
        in_specs=[hbm] * 6,
        out_specs=[hbm] * 12 + [pl.BlockSpec(memory_space=pltpu.VMEM)],
        scratch_shapes=[
            row_t(*w_qkv.shape), row_t(*w_out.shape), row_t(*w_up.shape), row_t(*w_down.shape),
            row_t(units, rows, width), row_t(units, rows, width), row_t(2, rows, width), row_t(2, rows, width), row_t(rows, width),
            row_t(rows, width), row_t(2, rows, 3 * width), row_t(rows, width), row_t(2, rows, width), row_t(rows, width),
            row_t(2, rows, ff), row_t(rows, ff), row_t(rows, ff), row_t(rows, width), row_t(rows, width), row_t(rows, 3 * width),
            dma((4,)), dma((units,)), dma, dma((2,)), dma((units,)), dma((2,)), dma((units,)), dma((7,)), dma((4,)), dma((3,)),
        ],
        compiler_params=pltpu.CompilerParams(collective_id=0, has_side_effects=True, vmem_limit_bytes=67043328),
        name="pipeline",
    )(embeds, targets, w_qkv, w_out, w_up, w_down)


def solution(mesh):
    num_stages = mesh.shape["stage"]

    def stage_program(embeds, targets, w_qkv, w_out, w_up, w_down):
        num_micro, batch_size, seq_len, model_dim = embeds.shape
        num_heads, head_dim = w_out.shape[1], w_out.shape[2]
        flat = (num_micro * batch_size, seq_len, model_dim)
        res = run_pipeline(
            "stage", num_stages, embeds.reshape(flat), targets.reshape(flat),
            w_qkv[0], w_out[0].reshape(num_heads * head_dim, model_dim), w_up[0], w_down[0], head_dim)
        xn, ctx, z, gl, dqkv, dh, dpre, g, dx = res[:9]
        loss = res[-1]
        grad_w = lambda a, b: jnp.einsum("usd,use->de", a, b, preferred_element_type=F32)
        is_first = lax.axis_index("stage") == 0
        is_last = lax.axis_index("stage") == num_stages - 1
        dx = lax.psum(jnp.where(is_first, dx, jnp.zeros_like(dx)), "stage")
        total = lax.psum(jnp.where(is_last, jnp.sum(loss), 0.0), "stage").reshape(1)
        return (
            total,
            grad_w(xn, dqkv)[None],
            grad_w(ctx, dh).reshape(w_out.shape),
            grad_w(z, dpre)[None],
            grad_w(gl, g)[None],
            dx.reshape(embeds.shape),
        )

    act_spec = P("rep", None, None, None)
    w3_spec = P("stage", None, None)
    g3_spec = P(("rep", "stage"), None, None)
    in_specs = (act_spec, act_spec, w3_spec, P("stage", None, None, None), w3_spec, w3_spec)
    out_specs = (P("rep"), g3_spec, P(("rep", "stage"), None, None, None), g3_spec, g3_spec, act_spec)
    return jax.shard_map(stage_program, mesh=mesh, in_specs=in_specs, out_specs=out_specs, check_vma=False)
```

```python
import functools

import jax
import jax.numpy as jnp
from jax import lax
from jax.experimental import pallas as pl
from jax.experimental.pallas import tpu as pltpu
from jax.sharding import PartitionSpec as P


F32, BF16 = jnp.float32, jnp.bfloat16
MESH = pl.DeviceIdType.MESH
NORM_EPS = 1e-6
NEG_BIG = -1e30
GELU_SCALE, GELU_CUBE = 0.7978845608028654, 0.044715
LANE = 128
NORM_ROWS = 32
RING = 4
VMEM_BYTES = 67043328


def mm(lhs, rhs):
    return jnp.dot(lhs, rhs, preferred_element_type=F32)


def mm_rt(lhs, rhs):
    return lax.dot_general(lhs, rhs, (((1,), (1,)), ((), ())), preferred_element_type=F32)


def mm_lt(lhs, rhs):
    return lax.dot_general(lhs, rhs, (((0,), (0,)), ((), ())), preferred_element_type=F32)


def cols(ref, lo, hi):
    return jnp.concatenate([ref[j] for j in range(lo, hi)], 1)


def rows_of(ref, lo, hi):
    return jnp.concatenate([ref[j, lo:hi, :] for j in range(ref.shape[0])], 1)


def pieces(vals):
    return [vals[:, LANE * j : LANE * j + LANE] for j in range(vals.shape[1] // LANE)]


def put(ref, lo, vals):
    for j, piece in enumerate(pieces(vals)):
        ref[lo + j] = piece


def accumulate(ref, vals, first):
    for j, piece in enumerate(pieces(vals)):
        ref[j] = piece if first else ref[j] + piece


def transpose_into(dst, src, lo, hi):
    for j in range(lo, hi):
        flipped = src[j].T
        for t, piece in enumerate(pieces(flipped)):
            dst[t, LANE * j : LANE * j + LANE, :] = piece


def row_scale(sums, width):
    return jnp.sum(sums, axis=-1, keepdims=True) * (1.0 / width)


def norm_into(dst, load):
    blocks, height = dst.shape[0], dst.shape[1]
    for r in range(0, height, NORM_ROWS):
        vals = [load(j, r) for j in range(blocks)]
        total = sum(v * v for v in vals)
        scale = lax.rsqrt(row_scale(total, blocks * LANE) + NORM_EPS)
        for j, v in enumerate(vals):
            dst[j, r : r + NORM_ROWS, :] = (v * scale).astype(BF16)


def norm_vjp_into(dst, base, load, d_load):
    blocks, height = dst.shape[0], dst.shape[1]
    width = blocks * LANE
    for r in range(0, height, NORM_ROWS):
        vals = [load(j, r) for j in range(blocks)]
        grads = [d_load(j, r) for j in range(blocks)]
        scale = lax.rsqrt(row_scale(sum(v * v for v in vals), width) + NORM_EPS)
        pull = scale * scale * scale * row_scale(sum(v * d for v, d in zip(vals, grads)), width)
        for j in range(blocks):
            dst[j, r : r + NORM_ROWS, :] = (base(j, r) + (grads[j] * scale - vals[j] * pull)).astype(BF16)


def reader(ref):
    return lambda j, r: ref[j, r : r + NORM_ROWS, :].astype(F32)


def rounded(ref):
    return lambda j, r: ref[j, r : r + NORM_ROWS, :].astype(BF16).astype(F32)


def gelu(x):
    t = jnp.tanh(x * (GELU_SCALE + (GELU_SCALE * GELU_CUBE) * (x * x)))
    return (0.5 * x) * (1.0 + t)


def gelu_grad(x):
    x_sq = x * x
    t = jnp.tanh(x * (GELU_SCALE + (GELU_SCALE * GELU_CUBE) * x_sq))
    up = 1.0 + t
    return 0.5 * (up + (((1.0 - t) * up) * x) * (GELU_SCALE + (3 * GELU_SCALE * GELU_CUBE) * x_sq))


def head_half(vals, which):
    lane = lax.broadcasted_iota(jnp.int32, (1, LANE), 1)
    return jnp.where((lane < LANE // 2) if which == 0 else (lane >= LANE // 2), vals, jnp.zeros_like(vals))


def split_heads(vals):
    return [head_half(vals, 0), head_half(vals, 1)]


def pair_scores(keys, queries):
    n = LANE
    return mm_rt(keys[:n], queries[:n]), mm_rt(keys, queries[n:])


def column_softmax(scores):
    e = jnp.exp(scores - jnp.max(scores, axis=0, keepdims=True))
    return e * (1.0 / jnp.sum(e, axis=0, keepdims=True))


def probs(scores, causal, scale):
    n = LANE
    s0, s1 = ((s * scale).astype(BF16).astype(F32) for s in scores)
    s0 = jnp.where(causal, s0, NEG_BIG)
    s1 = jnp.concatenate([s1[:n], jnp.where(causal, s1[n:], NEG_BIG)], 0)
    return column_softmax(s0), column_softmax(s1)


def causal_mask():
    return lax.broadcasted_iota(jnp.int32, (LANE, LANE), 0) <= lax.broadcasted_iota(jnp.int32, (LANE, LANE), 1)


def layer_forward(x, w_qkv, w_out, w_up, w_down, u, qkv, ctx_t, hid, pre, gl, out, acc, u_t, z_t, gl_t, scale, marks):
    blocks = x.shape[0]
    ff_blocks = w_up.shape[0]
    quads = blocks // 2
    half = LANE // 2
    causal = causal_mask()
    norm_into(u, reader(x))

    def project(i):
        for w in range(3):
            lo = w * blocks + 2 * i
            put(qkv, lo, mm(cols(u, 0, blocks), cols(w_qkv, lo, lo + 2)).astype(BF16))

    def out_part(lo, hi):
        return mm_lt(jnp.concatenate([ctx_t[0, lo:hi, :], ctx_t[1, lo:hi, :]], 1), rows_of(w_out, lo, hi))

    project(0)
    transpose_into(u_t, u, 0, blocks)
    for i in range(quads):
        pairs = (2 * i, 2 * i + 1)
        scores = [pair_scores(k, qkv[p]) for p in pairs for k in split_heads(qkv[blocks + p])]
        if i < quads - 1:
            project(i + 1)
        else:
            marks["qkv"]()
            accumulate(acc, out_part(0, 2 * LANE * i), True)
        a = [probs(s, causal, scale) for s in scores]
        for j, p in enumerate(pairs):
            v_t = qkv[2 * blocks + p].T
            for h in range(2):
                a0, a1 = a[2 * j + h]
                rows = slice(LANE * p + half * h, LANE * p + half * h + half)
                v_head = v_t[half * h : half * h + half]
                ctx_t[0, rows, :] = mm(v_head[:, :LANE], a0.astype(BF16)).astype(BF16)
                ctx_t[1, rows, :] = mm(v_head, a1.astype(BF16)).astype(BF16)
    accumulate(acc, out_part(2 * LANE * (quads - 1), blocks * LANE), False)
    marks["ctx"]()
    for r in range(0, x.shape[1], NORM_ROWS):
        for j in range(blocks):
            hid[j, r : r + NORM_ROWS, :] = (x[j, r : r + NORM_ROWS, :].astype(F32) + acc[j, r : r + NORM_ROWS, :]).astype(BF16)
    norm_into(u, reader(hid))
    step = 4
    up = lambda c: mm(cols(u, 0, blocks), cols(w_up, c, c + step)).astype(BF16)
    cur = up(0)
    transpose_into(z_t, u, 0, blocks)
    for c in range(0, ff_blocks, step):
        nxt = up(c + step) if c + step < ff_blocks else None
        for j, piece in enumerate(pieces(cur)):
            pre[c + j] = piece
            gl[c + j] = gelu(piece.astype(F32)).astype(BF16)
        transpose_into(gl_t, gl, c, c + step)
        cur = nxt
    marks["ff"]()
    for j, piece in enumerate(pieces(mm(cols(gl, 0, ff_blocks), cols(w_down, 0, blocks)))):
        out[j] = (hid[j].astype(F32) + piece).astype(BF16)


def layer_backward(g, x, hid, qkv, pre, w_qkv, w_out, w_up, w_down, d_qkv, d_ctx, d_hid, d_pre, out, acc, scale, marks):
    blocks = x.shape[0]
    ff_blocks = w_up.shape[0]
    quads = blocks // 2
    half = LANE // 2
    causal = causal_mask()
    step = 4
    down = lambda c: mm_rt(cols(g, 0, blocks), rows_of(w_down, LANE * c, LANE * (c + step))).astype(BF16)
    cur = down(0)
    for c in range(0, ff_blocks, step):
        nxt = down(c + step) if c + step < ff_blocks else None
        for j, piece in enumerate(pieces(cur)):
            d_pre[c + j] = (piece.astype(F32) * gelu_grad(pre[c + j].astype(F32))).astype(BF16)
        accumulate(acc, mm_rt(cols(d_pre, c, c + step), cols(w_up, c, c + step)), c == 0)
        cur = nxt
    norm_vjp_into(d_hid, reader(g), reader(hid), rounded(acc))
    marks["ff"]()

    def ctx_part(i):
        put(d_ctx, 2 * i, mm_rt(cols(d_hid, 0, blocks), rows_of(w_out, 2 * LANE * i, 2 * LANE * (i + 1))).astype(BF16))

    def qkv_part(i):
        take = lambda ref: jnp.concatenate([ref[w * blocks + 2 * i + t] for w in range(3) for t in range(2)], 1)
        accumulate(acc, mm_rt(take(d_qkv), take(w_qkv)), i == 0)

    ctx_part(0)
    for i in range(quads):
        pairs = (2 * i, 2 * i + 1)
        scores = [pair_scores(k, qkv[p]) for p in pairs for k in split_heads(qkv[blocks + p])]
        d_probs = [pair_scores(v, d_ctx[p]) for p in pairs for v in split_heads(qkv[2 * blocks + p])]
        if i < quads - 1:
            ctx_part(i + 1)
        if i > 0:
            qkv_part(i - 1)
        a, ds = [], []
        for s, dp in zip(scores, d_probs):
            a_pair = probs(s, causal, scale)
            dp = [d.astype(BF16).astype(F32) for d in dp]
            ds.append([(p * (d - jnp.sum(p * d, axis=0, keepdims=True))).astype(BF16) for p, d in zip(a_pair, dp)])
            a.append([p.astype(BF16) for p in a_pair])
        for j, p in enumerate(pairs):
            n = LANE

            def weigh(first, second, vals):
                top = mm(
                    jnp.concatenate([first[0], first[1][:n], second[0], second[1][:n]], 1), jnp.concatenate(vals, 0))
                low = mm(
                    jnp.concatenate([first[1][n:], second[1][n:]], 1), jnp.concatenate([vals[0][n:], vals[1][n:]], 0))
                return jnp.concatenate([top, low], 0)

            heads = (2 * j, 2 * j + 1)
            d_qkv[2 * blocks + p] = weigh(*(a[h] for h in heads), split_heads(d_ctx[p])).astype(BF16)
            d_qkv[blocks + p] = (weigh(*(ds[h] for h in heads), split_heads(qkv[p])) * scale).astype(BF16)
            k_t = qkv[blocks + p].T
            dq_t = []
            for h in range(2):
                k_head = k_t[half * h : half * h + half]
                d0, d1 = ds[heads[h]]
                dq_t.append(jnp.concatenate([mm(k_head[:, :n], d0), mm(k_head, d1)], 1) * scale)
            d_qkv[p] = jnp.concatenate(dq_t, 0).astype(BF16).T
    qkv_part(quads - 1)
    marks["qkv"]()
    norm_vjp_into(out, reader(d_hid), reader(x), rounded(acc))


def pipeline_kernel(
    axis, stages, units, scale, inv_count,
    embeds, targets, w_qkv_h, w_out_h, w_up_h, w_down_h,
    ut_all, ctx_all, zt_all, glt_all, dqkv_all, dh_all, dpre_all, g_all, dx_all, qkv_all, h_all, pre_all, x_all, loss,
    w_qkv, w_out, w_up, w_down, act, grad, out, d_in, target,
    u, qkv, ctx_t, hid, pre, gl, u_t, z_t, gl_t, acc, dpre, dh, dctx, dqkv,
    w_sem, emb_sem, tgt_sem, f_send, f_recv, f_free, b_send, b_recv, b_free, f_save, b_save, b_load,
):
    stage = lax.axis_index(axis)
    last = stages - 1
    blocks, height = act.shape[1], act.shape[2]
    right, left = lax.rem(stage + 1, stages), lax.rem(stage + last, stages)
    barrier = pltpu.get_barrier_semaphore()
    for neighbour in (left, right):
        pl.semaphore_signal(barrier, inc=1, device_id={axis: neighbour}, device_id_type=MESH)

    def load_columns(src, dst, sem):
        def start(j, carry):
            pltpu.make_async_copy(src.at[:, pl.ds(pl.multiple_of(j * LANE, LANE), LANE)], dst.at[j], sem).start()
            return carry

        lax.fori_loop(0, dst.shape[0], start, 0)

    def wait_whole(ref, sem):
        pltpu.make_async_copy(ref, ref, sem).wait()

    def embed_slot(unit):
        return act.at[lax.rem(unit, RING)], emb_sem.at[lax.rem(unit, RING)]

    def embed_start(unit):
        load_columns(embeds.at[unit], *embed_slot(unit))

    weights = ((w_qkv_h, w_qkv), (w_out_h, w_out), (w_up_h, w_up), (w_down_h, w_down))

    @pl.when(stage == 0)
    def _():
        embed_start(0)

    for i, (src, dst) in enumerate(weights):
        load_columns(src, dst, w_sem.at[i])

    @pl.when(stage == 0)
    def _():
        embed_start(1)

    pl.semaphore_wait(barrier, 2)
    loss[...] = jnp.zeros_like(loss)

    def f_copy(unit):
        slot, ring = lax.rem(unit, 2), lax.rem(unit, RING)
        return pltpu.make_async_remote_copy(
            src_ref=out.at[slot], dst_ref=act.at[ring], send_sem=f_send.at[slot], recv_sem=f_recv.at[ring],
            device_id={axis: right}, device_id_type=MESH)

    def b_copy(unit):
        slot, ring = lax.rem(unit, 2), lax.rem(unit, RING)
        return pltpu.make_async_remote_copy(
            src_ref=d_in.at[slot], dst_ref=grad.at[ring], send_sem=b_send.at[slot], recv_sem=b_recv.at[ring],
            device_id={axis: left}, device_id_type=MESH)

    def dx_copy(unit):
        slot = lax.rem(unit, 2)
        return pltpu.make_async_copy(d_in.at[slot], dx_all.at[unit], b_send.at[slot])

    def f_saves(unit):
        pairs = (
            (act.at[lax.rem(unit, RING)], x_all), (u_t, ut_all), (qkv.at[0], qkv_all), (ctx_t, ctx_all),
            (hid.at[0], h_all), (z_t, zt_all), (pre.at[0], pre_all), (gl_t, glt_all))
        return [pltpu.make_async_copy(src, dst.at[unit], f_save.at[i]) for i, (src, dst) in enumerate(pairs)]

    def b_saves(unit):
        pairs = ((grad.at[lax.rem(unit, RING)], g_all), (dpre, dpre_all), (dh, dh_all), (dqkv, dqkv_all))
        return [pltpu.make_async_copy(src, dst.at[unit], b_save.at[i]) for i, (src, dst) in enumerate(pairs)]

    def b_loads(unit):
        pairs = (
            (pre_all, pre.at[1]), (h_all, hid.at[1]), (qkv_all, qkv.at[1]), (x_all, act.at[RING + lax.rem(unit, 2)]))
        return [pltpu.make_async_copy(src.at[unit], dst, b_load.at[i]) for i, (src, dst) in enumerate(pairs)]

    def forward(unit):
        ring, slot = lax.rem(unit, RING), lax.rem(unit, 2)
        saves = f_saves(unit)

        @pl.when(stage == last)
        def _():
            load_columns(targets.at[unit], target, tgt_sem)

        @pl.when((stage == 0) & (unit + 2 < units))
        def _():
            embed_start(unit + 2)

        @pl.when(stage == 0)
        def _():
            wait_whole(*embed_slot(unit))

        @pl.when(stage > 0)
        def _():
            f_copy(unit).wait_recv()

        @pl.when(unit == 0)
        def _():
            wait_whole(w_qkv, w_sem.at[0])

        saves[0].start()

        def qkv_ready():
            @pl.when(unit == 0)
            def _():
                wait_whole(w_out, w_sem.at[1])

            saves[1].start()
            saves[2].start()

        def ctx_ready():
            @pl.when(unit == 0)
            def _():
                wait_whole(w_up, w_sem.at[2])
                wait_whole(w_down, w_sem.at[3])

            saves[3].start()

        def ff_ready():
            for i in range(4, 8):
                saves[i].start()

            @pl.when((stage < last) & (unit >= 2))
            def _():
                f_copy(unit).wait_send()

            @pl.when((stage < last) & (unit >= RING))
            def _():
                pl.semaphore_wait(f_free, 1)

        layer_forward(
            act.at[ring], w_qkv, w_out, w_up, w_down, u, qkv.at[0], ctx_t, hid.at[0], pre.at[0], gl, out.at[slot], acc,
            u_t, z_t, gl_t, scale, {"qkv": qkv_ready, "ctx": ctx_ready, "ff": ff_ready})

        @pl.when(stage < last)
        def _():
            f_copy(unit).start()

        @pl.when(stage == last)
        def _():
            wait_whole(target, tgt_sem)
            part = jnp.zeros((8, LANE), F32)
            for j in range(blocks):
                err = out[slot, j].astype(F32) - target[j].astype(F32)
                grad[ring, j] = (err * inv_count).astype(BF16)
                part += jnp.sum((err * err).reshape(height // 8, 8, LANE), axis=0)
            loss[...] += part * (0.5 * inv_count)

    def backward(unit):
        ring, slot = lax.rem(unit, RING), lax.rem(unit, 2)
        src = jnp.where(stage == last, 0, 1)
        x_slot = jnp.where(stage == last, ring, RING + slot)
        saves = b_saves(unit)
        following = b_loads(unit + 1)
        more = (stage < last) & (unit + 1 < units)

        @pl.when(unit > 0)
        def _():
            for copy in b_saves(unit - 1):
                copy.wait()

            @pl.when((stage < last) & (unit - 1 < units - RING))
            def _():
                pl.semaphore_signal(b_free, inc=1, device_id={axis: right}, device_id_type=MESH)

        @pl.when(stage < last)
        def _():
            b_copy(unit).wait_recv()
            for copy in b_loads(unit):
                copy.wait()

        saves[0].start()

        def ff_ready():
            saves[1].start()
            saves[2].start()

            @pl.when(more)
            def _():
                for i in (0, 1, 3):
                    following[i].start()

        def qkv_ready():
            saves[3].start()

            @pl.when(more)
            def _():
                following[2].start()

            @pl.when(unit >= 2)
            def _():
                @pl.when(stage > 0)
                def _():
                    b_copy(unit).wait_send()

                @pl.when(stage == 0)
                def _():
                    dx_copy(unit).wait()

            @pl.when((stage > 0) & (unit >= RING))
            def _():
                pl.semaphore_wait(b_free, 1)

        layer_backward(
            grad.at[ring], act.at[x_slot], hid.at[src], qkv.at[src], pre.at[src], w_qkv, w_out, w_up, w_down,
            dqkv, dctx, dh, dpre, d_in.at[slot], acc, scale, {"ff": ff_ready, "qkv": qkv_ready})

        @pl.when(stage > 0)
        def _():
            b_copy(unit).start()

        @pl.when(stage == 0)
        def _():
            dx_copy(unit).start()

    def tick(t, carry):
        f_unit = t - stage
        b_unit = t - 2 * last + stage

        @pl.when((f_unit >= 1) & (f_unit <= units))
        def _():
            for copy in f_saves(f_unit - 1):
                copy.wait()

            @pl.when((stage > 0) & (f_unit - 1 < units - RING))
            def _():
                pl.semaphore_signal(f_free, inc=1, device_id={axis: left}, device_id_type=MESH)

        @pl.when((stage < last) & (b_unit == 0))
        def _():
            for copy in b_loads(0):
                copy.start()

        @pl.when((f_unit >= 0) & (f_unit < units))
        def _():
            forward(f_unit)

        @pl.when((b_unit >= 0) & (b_unit < units))
        def _():
            backward(b_unit)

        return carry

    lax.fori_loop(0, units + 2 * last, tick, 0)

    for copy in b_saves(units - 1):
        copy.wait()

    for unit in (units - 2, units - 1):
        @pl.when(stage < last)
        def _():
            f_copy(unit).wait_send()

        @pl.when(stage > 0)
        def _():
            b_copy(unit).wait_send()

        @pl.when(stage == 0)
        def _():
            dx_copy(unit).wait()


def run_pipeline(axis, stages, embeds, targets, w_qkv, w_out, w_up, w_down, head_dim):
    units, height, width = embeds.shape
    n, ff = width // LANE, w_up.shape[1] // LANE
    halves = height // LANE
    saved = lambda *shape: jax.ShapeDtypeStruct((units,) + shape, BF16)
    rows_t = lambda k: saved(k, height, LANE)
    cols_t = lambda k: saved(halves, k, LANE)
    hbm = pl.BlockSpec(memory_space=pl.ANY)
    vm = lambda *shape: pltpu.VMEM(shape, BF16)
    rows = lambda *lead: vm(*lead, height, LANE)
    dma = pltpu.SemaphoreType.DMA
    outs = [
        cols_t(width), cols_t(width), cols_t(width), cols_t(ff * LANE), rows_t(3 * n), rows_t(n), rows_t(ff), rows_t(n), rows_t(n),
        rows_t(3 * n), rows_t(n), rows_t(ff), rows_t(n), jax.ShapeDtypeStruct((8, LANE), F32)]
    return pl.pallas_call(
        functools.partial(pipeline_kernel, axis, stages, units, head_dim ** -0.5, 1.0 / (units * height * width)),
        out_shape=outs,
        in_specs=[hbm] * 6,
        out_specs=[hbm] * 13 + [pl.BlockSpec(memory_space=pltpu.VMEM)],
        scratch_shapes=[
            vm(3 * n, width, LANE), vm(n, width, LANE), vm(ff, width, LANE), vm(n, ff * LANE, LANE),
            rows(RING + 2, n), rows(RING, n), rows(2, n), rows(2, n), rows(n),
            rows(n), rows(2, 3 * n), vm(halves, width, LANE), rows(2, n), rows(2, ff), rows(ff),
            vm(halves, width, LANE), vm(halves, width, LANE), vm(halves, ff * LANE, LANE),
            pltpu.VMEM((n, height, LANE), F32), rows(ff), rows(n), rows(n), rows(3 * n),
            dma((4,)), dma((RING,)), dma, dma((2,)), dma((RING,)), pltpu.SemaphoreType.REGULAR,
            dma((2,)), dma((RING,)), pltpu.SemaphoreType.REGULAR, dma((8,)), dma((4,)), dma((4,)),
        ],
        compiler_params=pltpu.CompilerParams(collective_id=0, has_side_effects=True, vmem_limit_bytes=VMEM_BYTES),
        name="pipeline",
    )(embeds, targets, w_qkv, w_out, w_up, w_down)


TILE_M, TILE_N = 1024, 512


def weight_kernel(left_refs, right_refs, out_refs, lefts, rights, tiles, l_sem, r_sem, o_sem):
    plan, left_plan = [], []
    for w, (a, b) in enumerate(zip(left_refs, right_refs)):
        m_tiles, n_tiles = a.shape[2] // TILE_M, b.shape[1] * LANE // TILE_N
        for m in range(m_tiles):
            left_plan.append((w, m, len(plan)))
            plan += [(w, m, n) for n in range(n_tiles)]
    steps, per = len(plan), TILE_N // LANE

    def left_copy(i):
        w, m, _ = left_plan[i]
        return pltpu.make_async_copy(left_refs[w].at[:, :, pl.ds(m * TILE_M, TILE_M), :], lefts.at[i % 2], l_sem.at[i % 2])

    spans = []
    for w, m, first in left_plan:
        spans.append((w, m, first, sum(1 for p in plan if p[:2] == (w, m))))

    def right_copy(step):
        for w, m, first, count in spans:
            @pl.when((step >= first) & (step < first + count))
            def _():
                slot = lax.rem(step, 2)
                pltpu.make_async_copy(
                    right_refs[w].at[:, pl.ds((step - first) * per, per)], rights.at[slot], r_sem.at[slot]).start()

    def out_copy(step):
        for w, m, first, count in spans:
            @pl.when((step >= first) & (step < first + count))
            def _():
                slot = lax.rem(step, 2)
                at = pl.multiple_of((step - first) * TILE_N, TILE_N)
                pltpu.make_async_copy(
                    tiles.at[slot], out_refs[w].at[pl.ds(m * TILE_M, TILE_M), pl.ds(at, TILE_N)], o_sem.at[slot]).start()

    def wait_out(slot):
        pltpu.make_async_copy(tiles.at[slot], tiles.at[slot], o_sem.at[slot]).wait()

    left_copy(0).start()
    right_copy(0)
    left_copy(1).start()

    def body(step, phase):
        slot = lax.rem(step, 2)

        @pl.when(step + 1 < steps)
        def _():
            right_copy(step + 1)

        fresh = functools.reduce(jnp.logical_or, [step == first for _, _, first, _ in spans])
        phase = phase + jnp.where(fresh, 1, 0)
        for i, (_, _, first, _) in enumerate(spans):
            @pl.when(step == first)
            def _():
                left_copy(i).wait()
                if 0 < i < len(spans) - 1:
                    left_copy(i + 1).start()

        pltpu.make_async_copy(rights.at[slot], rights.at[slot], r_sem.at[slot]).wait()

        @pl.when(step >= 2)
        def _():
            wait_out(slot)

        units, halves = lefts.shape[1], lefts.shape[2]
        a_ref, b_ref = lefts.at[lax.rem(phase, 2)], rights.at[slot]
        a = jnp.concatenate([a_ref[k, t] for k in range(units) for t in range(halves)], 1)
        b = jnp.concatenate([jnp.concatenate([b_ref[k, j] for j in range(per)], 1) for k in range(units)], 0)
        tiles[slot] = mm(a, b)
        out_copy(step)
        return phase

    lax.fori_loop(0, steps, body, jnp.int32(-1))
    wait_out(0)
    wait_out(1)


def weight_grads(lefts, rights):
    units, halves, _, _ = lefts[0].shape
    height = rights[0].shape[2]
    hbm = pl.BlockSpec(memory_space=pl.ANY)
    dma = pltpu.SemaphoreType.DMA
    num = len(lefts)
    flops = sum(2 * units * height * a.shape[2] * b.shape[1] * LANE for a, b in zip(lefts, rights))

    def kernel(*refs):
        weight_kernel(refs[:num], refs[num : 2 * num], refs[2 * num : 3 * num], *refs[3 * num :])

    return pl.pallas_call(
        kernel,
        out_shape=[jax.ShapeDtypeStruct((a.shape[2], b.shape[1] * LANE), F32) for a, b in zip(lefts, rights)],
        in_specs=[hbm] * (2 * num),
        out_specs=[hbm] * num,
        scratch_shapes=[
            pltpu.VMEM((2, units, halves, TILE_M, LANE), BF16), pltpu.VMEM((2, units, TILE_N // LANE, height, LANE), BF16),
            pltpu.VMEM((2, TILE_M, TILE_N), F32), dma((2,)), dma((2,)), dma((2,))],
        compiler_params=pltpu.CompilerParams(vmem_limit_bytes=48 * 1024 * 1024),
        cost_estimate=pl.CostEstimate(flops=flops, bytes_accessed=200_000_000, transcendentals=0),
        name="weight_grads",
    )(*lefts, *rights)


def solution(mesh):
    num_stages = mesh.shape["stage"]

    def stage_program(embeds, targets, w_qkv, w_out, w_up, w_down):
        num_micro, batch_size, seq_len, model_dim = embeds.shape
        num_heads, head_dim = w_out.shape[1], w_out.shape[2]
        flat = (num_micro * batch_size, seq_len, model_dim)
        res = run_pipeline(
            "stage", num_stages, embeds.reshape(flat), targets.reshape(flat),
            w_qkv[0], w_out[0].reshape(num_heads * head_dim, model_dim), w_up[0], w_down[0], head_dim)
        u_t, ctx_t, z_t, gl_t, dqkv, dh, dpre, g, dx = res[:9]
        loss = res[-1]
        is_first = lax.axis_index("stage") == 0
        is_last = lax.axis_index("stage") == num_stages - 1
        dx = lax.psum(jnp.where(is_first, dx, jnp.zeros_like(dx)), "stage")
        total = lax.psum(jnp.where(is_last, jnp.sum(loss), 0.0), "stage").reshape(1)
        d_qkv, d_out, d_up, d_down = weight_grads((u_t, ctx_t, z_t, gl_t), (dqkv, dh, dpre, g))
        d_embeds = dx.transpose(0, 2, 1, 3).reshape(embeds.shape)
        return total, d_qkv[None], d_out.reshape(w_out.shape), d_up[None], d_down[None], d_embeds

    act_spec = P("rep", None, None, None)
    w3_spec = P("stage", None, None)
    g3_spec = P(("rep", "stage"), None, None)
    in_specs = (act_spec, act_spec, w3_spec, P("stage", None, None, None), w3_spec, w3_spec)
    out_specs = (P("rep"), g3_spec, P(("rep", "stage"), None, None, None), g3_spec, g3_spec, act_spec)
    return jax.shard_map(stage_program, mesh=mesh, in_specs=in_specs, out_specs=out_specs, check_vma=False)
```

```python
import functools

import jax
import jax.numpy as jnp
from jax import lax
from jax.experimental import pallas as pl
from jax.experimental.pallas import tpu as pltpu
from jax.sharding import PartitionSpec as P


F32, BF16 = jnp.float32, jnp.bfloat16
MESH = pl.DeviceIdType.MESH
NORM_EPS = 1e-6
NEG_BIG = -1e30
GELU_SCALE, GELU_CUBE = 0.7978845608028654, 0.044715
LANE = 128
NORM_ROWS = 32
RING = 3
TILE_M, TILE_N = 1024, 512
GROUP = 6
SPLIT_UNITS = 5
TILES_BETWEEN, TILES_AFTER = 4, 8
VMEM_BYTES = 67043328


def mm(lhs, rhs):
    return jnp.dot(lhs, rhs, preferred_element_type=F32)


def mm_rt(lhs, rhs):
    return lax.dot_general(lhs, rhs, (((1,), (1,)), ((), ())), preferred_element_type=F32)


def mm_lt(lhs, rhs):
    return lax.dot_general(lhs, rhs, (((0,), (0,)), ((), ())), preferred_element_type=F32)


def cols(ref, lo, hi):
    return jnp.concatenate([ref[j] for j in range(lo, hi)], 1)


def rows_of(ref, lo, hi):
    return jnp.concatenate([ref[j, lo:hi, :] for j in range(ref.shape[0])], 1)


def pieces(vals):
    return [vals[:, LANE * j : LANE * j + LANE] for j in range(vals.shape[1] // LANE)]


def put(ref, lo, vals):
    for j, piece in enumerate(pieces(vals)):
        ref[lo + j] = piece


def accumulate(ref, vals, first):
    for j, piece in enumerate(pieces(vals)):
        ref[j] = piece if first else ref[j] + piece


def row_scale(sums, width):
    return jnp.sum(sums, axis=-1, keepdims=True) * (1.0 / width)


def norm_into(dst, load, starts):
    blocks = dst.shape[0]
    for r in starts:
        vals = [load(j, r) for j in range(blocks)]
        total = sum(v * v for v in vals)
        scale = lax.rsqrt(row_scale(total, blocks * LANE) + NORM_EPS)
        for j, v in enumerate(vals):
            dst[j, r : r + NORM_ROWS, :] = (v * scale).astype(BF16)


def norm_vjp_into(dst, base, load, d_load):
    blocks, height = dst.shape[0], dst.shape[1]
    width = blocks * LANE
    for r in range(0, height, NORM_ROWS):
        vals = [load(j, r) for j in range(blocks)]
        grads = [d_load(j, r) for j in range(blocks)]
        scale = lax.rsqrt(row_scale(sum(v * v for v in vals), width) + NORM_EPS)
        pull = scale * scale * scale * row_scale(sum(v * d for v, d in zip(vals, grads)), width)
        for j in range(blocks):
            dst[j, r : r + NORM_ROWS, :] = (base(j, r) + (grads[j] * scale - vals[j] * pull)).astype(BF16)


def reader(ref):
    return lambda j, r: ref[j, r : r + NORM_ROWS, :].astype(F32)


def rounded(ref):
    return lambda j, r: ref[j, r : r + NORM_ROWS, :].astype(BF16).astype(F32)


def gelu(x):
    t = jnp.tanh(x * (GELU_SCALE + (GELU_SCALE * GELU_CUBE) * (x * x)))
    return (0.5 * x) * (1.0 + t)


def gelu_grad(x):
    x_sq = x * x
    t = jnp.tanh(x * (GELU_SCALE + (GELU_SCALE * GELU_CUBE) * x_sq))
    up = 1.0 + t
    return 0.5 * (up + (((1.0 - t) * up) * x) * (GELU_SCALE + (3 * GELU_SCALE * GELU_CUBE) * x_sq))


def head_half(vals, which):
    lane = lax.broadcasted_iota(jnp.int32, (1, LANE), 1)
    return jnp.where((lane < LANE // 2) if which == 0 else (lane >= LANE // 2), vals, jnp.zeros_like(vals))


def split_heads(vals):
    return [head_half(vals, 0), head_half(vals, 1)]


def pair_scores(keys, queries, halves=(0, 1)):
    return [mm_rt(keys[: LANE * (t + 1)], queries[LANE * t : LANE * (t + 1)]) for t in halves]


def column_softmax(scores):
    e = jnp.exp(scores - jnp.max(scores, axis=0, keepdims=True))
    return e * (1.0 / jnp.sum(e, axis=0, keepdims=True))


def probs(scores, causal, scale, halves=(0, 1)):
    parts = []
    for t, s in zip(halves, scores):
        s = (s * scale).astype(BF16).astype(F32)
        below = jnp.where(causal, s[LANE * t :], NEG_BIG)
        parts.append(column_softmax(jnp.concatenate([s[: LANE * t], below], 0) if t else below))
    return parts


def causal_mask():
    return lax.broadcasted_iota(jnp.int32, (LANE, LANE), 0) <= lax.broadcasted_iota(jnp.int32, (LANE, LANE), 1)


def skip():
    pass


def layer_forward(halves, x, w_qkv, w_out, w_up, w_down, u, qkv, ctx_t, hid, pre, gl, out, acc, u_t, z_t, gl_t, scale, marks):
    blocks = x.shape[0]
    ff_blocks = w_up.shape[0]
    quads = blocks // 2
    half = LANE // 2
    causal = causal_mask()
    rows = slice(LANE * halves[0], LANE * (halves[-1] + 1))
    starts = range(rows.start, rows.stop, NORM_ROWS)
    norm_into(u, reader(x), starts)

    def lhs(ref, lo, hi):
        return jnp.concatenate([ref[j, rows, :] for j in range(lo, hi)], 1)

    def store(ref, lo, vals):
        for j, piece in enumerate(pieces(vals)):
            ref[lo + j, rows, :] = piece

    def gather(vals, first):
        for j, piece in enumerate(pieces(vals)):
            acc[j, rows, :] = piece if first else acc[j, rows, :] + piece

    def flip(dsts, src, lo, hi):
        per = dsts[0].shape[1] // LANE
        for j in range(lo, hi):
            at = slice(LANE * (j % per), LANE * (j % per) + LANE)
            for t, piece in zip(halves, pieces(src[j, rows, :].T)):
                dsts[j // per][t, at, :] = piece

    def project(i):
        for w in range(3):
            lo = w * blocks + 2 * i
            store(qkv, lo, mm(lhs(u, 0, blocks), cols(w_qkv, lo, lo + 2)).astype(BF16))

    def out_part(lo, hi):
        return mm_lt(jnp.concatenate([ctx_t[t, lo:hi, :] for t in halves], 1), rows_of(w_out, lo, hi))

    project(0)
    flip([u_t], u, 0, blocks)
    for i in range(quads):
        pairs = (2 * i, 2 * i + 1)
        scores = [pair_scores(k, qkv[p], halves) for p in pairs for k in split_heads(qkv[blocks + p])]
        if i < quads - 1:
            project(i + 1)
        else:
            marks.get("qkv", skip)()
            gather(out_part(0, 2 * LANE * i), True)
        a = [probs(s, causal, scale, halves) for s in scores]
        for j, p in enumerate(pairs):
            v_t = qkv[2 * blocks + p].T
            for h in range(2):
                at = slice(LANE * p + half * h, LANE * p + half * h + half)
                v_head = v_t[half * h : half * h + half]
                for t, a_part in zip(halves, a[2 * j + h]):
                    ctx_t[t, at, :] = mm(v_head[:, : LANE * (t + 1)], a_part.astype(BF16)).astype(BF16)
    gather(out_part(2 * LANE * (quads - 1), blocks * LANE), False)
    marks.get("ctx", skip)()
    for r in starts:
        for j in range(blocks):
            at = slice(r, r + NORM_ROWS)
            hid[j, at, :] = (x[j, at, :].astype(F32) + acc[j, at, :]).astype(BF16)
    norm_into(u, reader(hid), starts)
    step = 4
    up = lambda c: mm(lhs(u, 0, blocks), cols(w_up, c, c + step)).astype(BF16)
    cur = up(0)
    flip([z_t], u, 0, blocks)
    for c in range(0, ff_blocks, step):
        nxt = up(c + step) if c + step < ff_blocks else None
        for j, piece in enumerate(pieces(cur)):
            pre[c + j, rows, :] = piece
            gl[c + j, rows, :] = gelu(piece.astype(F32)).astype(BF16)
        flip(gl_t, gl, c, c + step)
        cur = nxt
    marks.get("ff", skip)()
    for j, piece in enumerate(pieces(mm(lhs(gl, 0, ff_blocks), cols(w_down, 0, blocks)))):
        out[j, rows, :] = (hid[j, rows, :].astype(F32) + piece).astype(BF16)


def layer_backward(g, x, hid, qkv, pre, w_qkv, w_out, w_up, w_down, d_qkv, d_ctx, d_hid, d_pre, out, acc, scale, marks):
    blocks = x.shape[0]
    ff_blocks = w_up.shape[0]
    quads = blocks // 2
    half = LANE // 2
    causal = causal_mask()
    step = 4
    down = lambda c: mm_rt(cols(g, 0, blocks), rows_of(w_down, LANE * c, LANE * (c + step))).astype(BF16)
    cur = down(0)
    for c in range(0, ff_blocks, step):
        nxt = down(c + step) if c + step < ff_blocks else None
        for j, piece in enumerate(pieces(cur)):
            d_pre[c + j] = (piece.astype(F32) * gelu_grad(pre[c + j].astype(F32))).astype(BF16)
        accumulate(acc, mm_rt(cols(d_pre, c, c + step), cols(w_up, c, c + step)), c == 0)
        cur = nxt
    norm_vjp_into(d_hid, reader(g), reader(hid), rounded(acc))
    marks["ff"]()

    def ctx_part(i):
        put(d_ctx, 2 * i, mm_rt(cols(d_hid, 0, blocks), rows_of(w_out, 2 * LANE * i, 2 * LANE * (i + 1))).astype(BF16))

    def qkv_part(i):
        take = lambda ref: jnp.concatenate([ref[w * blocks + 2 * i + t] for w in range(3) for t in range(2)], 1)
        accumulate(acc, mm_rt(take(d_qkv), take(w_qkv)), i == 0)

    ctx_part(0)
    for i in range(quads):
        pairs = (2 * i, 2 * i + 1)
        scores = [pair_scores(k, qkv[p]) for p in pairs for k in split_heads(qkv[blocks + p])]
        d_probs = [pair_scores(v, d_ctx[p]) for p in pairs for v in split_heads(qkv[2 * blocks + p])]
        if i < quads - 1:
            ctx_part(i + 1)
        if i > 0:
            qkv_part(i - 1)
        a, ds = [], []
        for s, dp in zip(scores, d_probs):
            a_pair = probs(s, causal, scale)
            dp = [d.astype(BF16).astype(F32) for d in dp]
            ds.append([(p * (d - jnp.sum(p * d, axis=0, keepdims=True))).astype(BF16) for p, d in zip(a_pair, dp)])
            a.append([p.astype(BF16) for p in a_pair])
        for j, p in enumerate(pairs):
            n = LANE

            def weigh(first, second, vals):
                top = mm(
                    jnp.concatenate([first[0], first[1][:n], second[0], second[1][:n]], 1), jnp.concatenate(vals, 0))
                low = mm(
                    jnp.concatenate([first[1][n:], second[1][n:]], 1), jnp.concatenate([vals[0][n:], vals[1][n:]], 0))
                return jnp.concatenate([top, low], 0)

            heads = (2 * j, 2 * j + 1)
            d_qkv[2 * blocks + p] = weigh(*(a[h] for h in heads), split_heads(d_ctx[p])).astype(BF16)
            d_qkv[blocks + p] = (weigh(*(ds[h] for h in heads), split_heads(qkv[p])) * scale).astype(BF16)
            k_t = qkv[blocks + p].T
            dq_t = []
            for h in range(2):
                k_head = k_t[half * h : half * h + half]
                d0, d1 = ds[heads[h]]
                dq_t.append(jnp.concatenate([mm(k_head[:, :n], d0), mm(k_head, d1)], 1) * scale)
            d_qkv[p] = jnp.concatenate(dq_t, 0).astype(BF16).T
    qkv_part(quads - 1)
    marks["qkv"]()
    norm_vjp_into(out, reader(d_hid), reader(x), rounded(acc))


class WeightTiles:
    def __init__(self, left_refs, right_refs, acc_refs, out_refs, lefts, rights, tiles, l_sem, r_sem, a_sem, o_sem, first_unit, bare):
        self.left_refs, self.right_refs, self.acc_refs, self.out_refs = left_refs, right_refs, acc_refs, out_refs
        self.lefts, self.rights, self.tiles = lefts, rights, tiles
        self.l_sem, self.r_sem, self.a_sem, self.o_sem = l_sem, r_sem, a_sem, o_sem
        self.first_unit, self.bare = first_unit, bare
        self.units, self.halves = lefts.shape[1], lefts.shape[2]
        self.slots = tiles.shape[0]
        self.spans, self.steps = [], 0
        for w, (a, b) in enumerate(zip(left_refs, right_refs)):
            count = b.shape[1] * LANE // TILE_N
            for m in range(a.shape[2] // TILE_M):
                self.spans.append((w, m, self.steps, count))
                self.steps += count

    def group_units(self, group):
        return pl.ds(self.first_unit + group * self.units, self.units)

    def left_copy(self, k, group):
        w, m = self.spans[k][:2]
        src = self.left_refs[w].at[self.group_units(group), :, pl.ds(m * TILE_M, TILE_M), :]
        return pltpu.make_async_copy(src, self.lefts.at[k % 2], self.l_sem.at[k % 2])

    def each_span(self, j, fn):
        for w, m, first, count in self.spans:
            @pl.when((j >= first) & (j < first + count))
            def _():
                fn(w, m, j - first)

    def window(self, refs, w, m, n):
        return refs[w].at[pl.ds(m * TILE_M, TILE_M), pl.ds(pl.multiple_of(n * TILE_N, TILE_N), TILE_N)]

    def load(self, i):
        group, j = i // self.steps, lax.rem(i, self.steps)
        slot, tile = lax.rem(i, 2), lax.rem(i, self.slots)
        per = TILE_N // LANE

        @pl.when(i >= self.slots)
        def _():
            self.wait_store(tile)

        def start(w, m, n):
            src = self.right_refs[w].at[self.group_units(group), pl.ds(n * per, per)]
            pltpu.make_async_copy(src, self.rights.at[slot], self.r_sem.at[slot]).start()

            @pl.when(group >= self.bare)
            def _():
                pltpu.make_async_copy(
                    self.window(self.acc_refs, w, m, n), self.tiles.at[tile], self.a_sem.at[tile]).start()

        self.each_span(j, start)

    def wait_store(self, tile):
        pltpu.make_async_copy(self.tiles.at[tile], self.tiles.at[tile], self.o_sem.at[tile]).wait()

    def step(self, i):
        group, j = i // self.steps, lax.rem(i, self.steps)
        slot, tile = lax.rem(i, 2), lax.rem(i, self.slots)

        @pl.when(j == 0)
        def _():
            self.left_copy(0, group).start()
            self.load(i)
            self.left_copy(1, group).start()

        @pl.when(j + 1 < self.steps)
        def _():
            self.load(i + 1)

        chunk = -1
        for k, (_, _, first, _) in enumerate(self.spans):
            chunk = chunk + jnp.where(j >= first, 1, 0)

            @pl.when(j == first)
            def _():
                self.left_copy(k, group).wait()
                if 0 < k < len(self.spans) - 1:
                    self.left_copy(k + 1, group).start()

        pltpu.make_async_copy(self.rights.at[slot], self.rights.at[slot], self.r_sem.at[slot]).wait()

        @pl.when(group >= self.bare)
        def _():
            pltpu.make_async_copy(self.tiles.at[tile], self.tiles.at[tile], self.a_sem.at[tile]).wait()

        a_ref, b_ref = self.lefts.at[lax.rem(chunk, 2)], self.rights.at[slot]
        a = jnp.concatenate([a_ref[k, t] for k in range(self.units) for t in range(self.halves)], 1)
        b = jnp.concatenate([cols(b_ref.at[k], 0, TILE_N // LANE) for k in range(self.units)], 0)
        fresh = mm(a, b)
        if self.bare == 0:
            self.tiles[tile] = self.tiles[tile] + fresh
        else:
            self.tiles[tile] = jnp.where(group >= self.bare, self.tiles[tile], 0.0) + fresh

        def store(w, m, n):
            pltpu.make_async_copy(self.tiles.at[tile], self.window(self.out_refs, w, m, n), self.o_sem.at[tile]).start()

        self.each_span(j, store)


def pipeline_kernel(
    axis, stages, units, scale, inv_count,
    embeds, targets, w_qkv_h, w_out_h, w_up_h, w_down_h,
    ut_all, ctx_all, zt_all, glt_all, dqkv_all, dh_all, dpre_all, g_all, dx_all,
    gw_qkv, gw_out, gw_up, gw_down, qkv_all, h_all, pre_all, x_all, loss,
    w_qkv, w_out, w_up, w_down, act, grad, out, d_in,
    tmp_act, tmp_mid, tmp_ff, qkv, hid, pre, acc, dqkv, lefts, rights, tiles,
    w_sem, emb_sem, tgt_sem, f_send, f_recv, f_free, b_send, b_recv, b_free, f_save, b_save, b_load,
    x_send, x_recv, l_send, l_recv, wl_sem, wr_sem, wa_sem, wo_sem,
):
    stage = lax.axis_index(axis)
    last = stages - 1
    blocks, height = act.shape[1], act.shape[2]
    halves = range(height // LANE)
    right, left = lax.rem(stage + 1, stages), lax.rem(stage + last, stages)
    u = dctx = tmp_act
    target = dh = tmp_mid
    gl = dpre = tmp_ff
    chunks = w_down.shape[1] // TILE_M
    gl_t = [lefts.at[0, k] for k in range(chunks)]
    u_t, z_t, ctx_t = lefts.at[0, chunks], lefts.at[0, chunks + 1], lefts.at[1, 0]
    gw = (gw_qkv, gw_out, gw_up, gw_down)
    work = WeightTiles(
        (ut_all, ctx_all, zt_all, glt_all), (dqkv_all, dh_all, dpre_all, g_all), gw, gw, lefts, rights, tiles,
        wl_sem, wr_sem, wa_sem, wo_sem, 0, 1)
    groups = units // GROUP
    total_tiles = groups * work.steps
    barrier = pltpu.get_barrier_semaphore()
    for ahead in range(1, stages):
        pl.semaphore_signal(
            barrier, inc=1, device_id={axis: lax.rem(stage + ahead, stages)}, device_id_type=MESH)

    def load_columns(src, dst, sem):
        def start(j, carry):
            pltpu.make_async_copy(src.at[:, pl.ds(pl.multiple_of(j * LANE, LANE), LANE)], dst.at[j], sem).start()
            return carry

        lax.fori_loop(0, dst.shape[0], start, 0)

    def wait_whole(ref, sem):
        pltpu.make_async_copy(ref, ref, sem).wait()

    def embed_slot(unit):
        return act.at[lax.rem(unit, RING)], emb_sem.at[lax.rem(unit, RING)]

    def embed_start(unit):
        load_columns(embeds.at[unit], *embed_slot(unit))

    weights = ((w_qkv_h, w_qkv), (w_out_h, w_out), (w_up_h, w_up), (w_down_h, w_down))

    @pl.when(stage == 0)
    def _():
        embed_start(0)

    for i, (src, dst) in enumerate(weights):
        load_columns(src, dst, w_sem.at[i])

    @pl.when(stage == 0)
    def _():
        embed_start(1)

    loss[...] = jnp.zeros_like(loss)
    pl.semaphore_wait(barrier, last)

    def f_copy(unit, half):
        slot, ring = lax.rem(unit, 2), lax.rem(unit, RING)
        at = pl.ds(half * LANE, LANE)
        return pltpu.make_async_remote_copy(
            src_ref=out.at[slot, :, at, :], dst_ref=act.at[ring, :, at, :], send_sem=f_send.at[slot, half],
            recv_sem=f_recv.at[ring, half], device_id={axis: right}, device_id_type=MESH)

    def b_copy(unit):
        slot, ring = lax.rem(unit, 2), lax.rem(unit, RING)
        return pltpu.make_async_remote_copy(
            src_ref=d_in.at[slot], dst_ref=grad.at[ring], send_sem=b_send.at[slot], recv_sem=b_recv.at[ring],
            device_id={axis: left}, device_id_type=MESH)

    even = lax.rem(stage, 2) == 0
    chain = even & ((stage == 0) | (stage + 2 < stages - 2))
    branches = ((even, right), (chain, lax.rem(stage + 2, stages)), (stage == 0, stages - 2))

    def x_copies(unit, src):
        slot = lax.rem(unit, 2)
        return [
            (cond, pltpu.make_async_remote_copy(
                src_ref=src, dst_ref=dx_all.at[unit], send_sem=x_send.at[slot, k], recv_sem=x_recv.at[unit],
                device_id={axis: dest}, device_id_type=MESH))
            for k, (cond, dest) in enumerate(branches)]

    def x_start(unit, src):
        for cond, copy in x_copies(unit, src):
            @pl.when(cond)
            def _():
                copy.start()

    def x_wait_send(unit):
        for cond, copy in x_copies(unit, dx_all.at[unit]):
            @pl.when(cond)
            def _():
                copy.wait_send()

    def x_wait_recv(unit):
        x_copies(unit, dx_all.at[unit])[0][1].wait_recv()

    def dx_copy(unit):
        slot = lax.rem(unit, 2)
        return pltpu.make_async_copy(d_in.at[slot], dx_all.at[unit], b_send.at[slot])

    def loss_copy(k):
        return pltpu.make_async_remote_copy(
            src_ref=loss, dst_ref=loss, send_sem=l_send.at[k], recv_sem=l_recv, device_id={axis: k}, device_id_type=MESH)

    def f_saves(unit):
        pairs = [
            (act.at[lax.rem(unit, RING)], x_all.at[unit]), (u_t, ut_all.at[unit]), (qkv.at[0], qkv_all.at[unit]),
            (ctx_t, ctx_all.at[unit]), (hid.at[0], h_all.at[unit]), (z_t, zt_all.at[unit]), (pre.at[0], pre_all.at[unit])]
        pairs += [(ref, glt_all.at[unit, :, pl.ds(k * TILE_M, TILE_M), :]) for k, ref in enumerate(gl_t)]
        return [pltpu.make_async_copy(src, dst, f_save.at[i]) for i, (src, dst) in enumerate(pairs)]

    def b_saves(unit):
        pairs = ((grad.at[lax.rem(unit, RING)], g_all), (dqkv, dqkv_all), (dpre, dpre_all), (dh, dh_all))
        return [pltpu.make_async_copy(src, dst.at[unit], b_save.at[i]) for i, (src, dst) in enumerate(pairs)]

    def b_loads(unit):
        pairs = (
            (pre_all, pre.at[1]), (h_all, hid.at[1]), (qkv_all, qkv.at[1]), (x_all, act.at[RING + lax.rem(unit, 2)]))
        return [pltpu.make_async_copy(src.at[unit], dst, b_load.at[i]) for i, (src, dst) in enumerate(pairs)]

    def wait_late_saves(unit):
        for copy in b_saves(unit)[:2]:
            copy.wait()

    work_start = jnp.maximum(GROUP - 1 + 2 * last - stage, units + stage)
    b_end = units - 1 + 2 * last - stage

    def tiles_by(t):
        between = jnp.maximum(jnp.minimum(t, b_end) - work_start + 1, 0)
        return jnp.minimum(TILES_BETWEEN * between + TILES_AFTER * jnp.maximum(t - b_end, 0), total_tiles)

    def make_tiles(first, end):
        lax.fori_loop(first, end, lambda i, c: (work.step(i), c)[1], 0)

    def forward(unit):
        ring, slot = lax.rem(unit, RING), lax.rem(unit, 2)
        saves = f_saves(unit)

        @pl.when(stage == last)
        def _():
            load_columns(targets.at[unit], target, tgt_sem)

        @pl.when((stage == 0) & (unit + 2 < units))
        def _():
            embed_start(unit + 2)

        @pl.when((stage < last) & (unit >= 2))
        def _():
            for half in halves:
                f_copy(unit, half).wait_send()

        def run(part, marks):
            layer_forward(
                part, act.at[ring], w_qkv, w_out, w_up, w_down, u, qkv.at[0], ctx_t, hid.at[0], pre.at[0], gl,
                out.at[slot], acc, u_t, z_t, gl_t, scale, marks)

        def arrive(half):
            @pl.when((stage == 0) & (half == 0))
            def _():
                wait_whole(*embed_slot(unit))

            @pl.when(stage > 0)
            def _():
                f_copy(unit, half).wait_recv()

        def leave(half):
            @pl.when(stage < last)
            def _():
                f_copy(unit, half).start()

        def credit():
            @pl.when((stage < last) & (unit >= RING))
            def _():
                pl.semaphore_wait(f_free, 1)

        def weights_ready(*which):
            def wait():
                @pl.when(unit == 0)
                def _():
                    for w in which:
                        wait_whole(weights[w][1], w_sem.at[w])

            return wait

        @pl.when(unit < SPLIT_UNITS)
        def _():
            arrive(0)
            weights_ready(0)()
            run((0,), {"qkv": weights_ready(1), "ctx": weights_ready(2), "ff": weights_ready(3)})
            credit()
            leave(0)
            arrive(1)
            run((1,), {})
            leave(1)

        @pl.when(unit >= SPLIT_UNITS)
        def _():
            arrive(0)
            arrive(1)
            run((0, 1), {})
            credit()
            leave(0)
            leave(1)

        for copy in saves:
            copy.start()

        @pl.when(stage == last)
        def _():
            wait_whole(target, tgt_sem)
            part = jnp.zeros((8, LANE), F32)
            for j in range(blocks):
                err = out[slot, j].astype(F32) - target[j].astype(F32)
                grad[ring, j] = (err * inv_count).astype(BF16)
                part += jnp.sum((err * err).reshape(height // 8, 8, LANE), axis=0)
            loss[...] += part * (0.5 * inv_count)

        @pl.when((stage == last) & (unit == units - 1))
        def _():
            for k in range(stages - 1):
                loss_copy(k).start()

    def backward(unit, saved):
        ring, slot = lax.rem(unit, RING), lax.rem(unit, 2)
        src = jnp.where(stage == last, 0, 1)
        x_slot = jnp.where(stage == last, ring, RING + slot)
        saves = b_saves(unit)
        following = b_loads(unit + 1)
        more = (stage < last) & (unit + 1 < units)

        @pl.when(unit > 0)
        def _():
            @pl.when(jnp.logical_not(saved))
            def _():
                wait_late_saves(unit - 1)

            @pl.when((stage < last) & (unit - 1 < units - RING))
            def _():
                pl.semaphore_signal(b_free, inc=1, device_id={axis: right}, device_id_type=MESH)

        @pl.when(unit >= 2)
        def _():
            @pl.when(stage > 0)
            def _():
                b_copy(unit).wait_send()

            @pl.when(stage == 0)
            def _():
                dx_copy(unit).wait()
                x_wait_send(unit)

        @pl.when(stage < last)
        def _():
            b_copy(unit).wait_recv()
            for copy in b_loads(unit):
                copy.wait()

        saves[0].start()

        def ff_ready():
            saves[2].start()
            saves[3].start()

            @pl.when(more)
            def _():
                for i in (0, 1, 3):
                    following[i].start()

        def qkv_ready():
            saves[1].start()

            @pl.when(more)
            def _():
                following[2].start()

        layer_backward(
            grad.at[ring], act.at[x_slot], hid.at[src], qkv.at[src], pre.at[src], w_qkv, w_out, w_up, w_down,
            dqkv, dctx, dh, dpre, d_in.at[slot], acc, scale, {"ff": ff_ready, "qkv": qkv_ready})

        @pl.when((stage > 0) & (unit >= RING))
        def _():
            pl.semaphore_wait(b_free, 1)

        @pl.when(stage > 0)
        def _():
            b_copy(unit).start()

        @pl.when(stage == 0)
        def _():
            dx_copy(unit).start()
            x_start(unit, d_in.at[slot])

        saves[2].wait()
        saves[3].wait()

    def tick(t, carry):
        f_unit = t - stage
        b_unit = t - 2 * last + stage
        before, first, end = tiles_by(t - 2), tiles_by(t - 1), tiles_by(t)

        @pl.when((f_unit >= 1) & (f_unit <= units))
        def _():
            for copy in f_saves(f_unit - 1):
                copy.wait()

            @pl.when((stage > 0) & (f_unit - 1 < units - RING))
            def _():
                pl.semaphore_signal(f_free, inc=1, device_id={axis: left}, device_id_type=MESH)

        @pl.when((stage < last) & (b_unit == 0))
        def _():
            for copy in b_loads(0):
                copy.start()

        @pl.when((f_unit >= 0) & (f_unit < units))
        def _():
            forward(f_unit)

        @pl.when((b_unit >= 0) & (b_unit < units))
        def _():
            backward(b_unit, first > before)

            @pl.when(end > first)
            def _():
                wait_late_saves(b_unit)

        make_tiles(first, end)
        x_unit = t - 2 * last

        @pl.when(even & (stage > 0) & (x_unit >= 0))
        def _():
            x_wait_recv(x_unit)

            @pl.when(x_unit >= 2)
            def _():
                x_wait_send(x_unit)

            x_start(x_unit, dx_all.at[x_unit])

        return carry

    ticks = units + 2 * last
    lax.fori_loop(0, ticks, tick, 0)

    @pl.when(tiles_by(b_end) == tiles_by(b_end - 1))
    def _():
        wait_late_saves(units - 1)

    make_tiles(tiles_by(ticks - 1), total_tiles)

    for tile in range(work.slots):
        work.wait_store(tile)

    for unit in (units - 2, units - 1):
        @pl.when(stage < last)
        def _():
            for half in halves:
                f_copy(unit, half).wait_send()

        @pl.when(stage > 0)
        def _():
            b_copy(unit).wait_send()

        @pl.when(stage == 0)
        def _():
            dx_copy(unit).wait()

        x_wait_send(unit)

    @pl.when(jnp.logical_not(even))
    def _():
        lax.fori_loop(0, units, lambda unit, c: (x_wait_recv(unit), c)[1], 0)

    @pl.when(stage < last)
    def _():
        loss_copy(0).wait_recv()

    @pl.when(stage == last)
    def _():
        for k in range(stages - 1):
            loss_copy(k).wait_send()


def run_pipeline(axis, stages, embeds, targets, w_qkv, w_out, w_up, w_down, head_dim):
    units, height, width = embeds.shape
    n, ff = width // LANE, w_up.shape[1] // LANE
    halves = height // LANE
    saved = lambda *shape: jax.ShapeDtypeStruct((units,) + shape, BF16)
    rows_t = lambda k: saved(k, height, LANE)
    cols_t = lambda k: saved(halves, k, LANE)
    hbm = pl.BlockSpec(memory_space=pl.ANY)
    vm = lambda *shape: pltpu.VMEM(shape, BF16)
    rows = lambda *lead: vm(*lead, height, LANE)
    dma, regular = pltpu.SemaphoreType.DMA, pltpu.SemaphoreType.REGULAR
    outs = [
        cols_t(width), cols_t(width), cols_t(width), cols_t(ff * LANE), rows_t(3 * n), rows_t(n), rows_t(ff), rows_t(n), rows_t(n)]
    outs += [jax.ShapeDtypeStruct(w.shape, F32) for w in (w_qkv, w_out, w_up, w_down)]
    outs += [rows_t(3 * n), rows_t(n), rows_t(ff), rows_t(n), jax.ShapeDtypeStruct((8, LANE), F32)]
    return pl.pallas_call(
        functools.partial(pipeline_kernel, axis, stages, units, head_dim ** -0.5, 1.0 / (units * height * width)),
        out_shape=outs,
        in_specs=[hbm] * 6,
        out_specs=[hbm] * 17 + [pl.BlockSpec(memory_space=pltpu.VMEM)],
        scratch_shapes=[
            vm(3 * n, width, LANE), vm(n, width, LANE), vm(ff, width, LANE), vm(n, ff * LANE, LANE),
            rows(RING + 2, n), rows(RING, n), rows(2, n), rows(2, n),
            rows(n), rows(n), rows(ff), rows(2, 3 * n), rows(2, n), rows(2, ff), pltpu.VMEM((n, height, LANE), F32), rows(3 * n),
            vm(2, GROUP, halves, TILE_M, LANE), rows(2, GROUP, TILE_N // LANE), pltpu.VMEM((3, TILE_M, TILE_N), F32),
            dma((4,)), dma((RING,)), dma, dma((2, halves)), dma((RING, halves)), regular,
            dma((2,)), dma((RING,)), regular, dma((7 + ff * LANE // TILE_M,)), dma((4,)), dma((4,)),
            dma((2, 3)), dma((units,)), dma((stages - 1,)), dma, dma((2,)), dma((2,)), dma((3,)), dma((3,)),
        ],
        compiler_params=pltpu.CompilerParams(collective_id=0, has_side_effects=True, vmem_limit_bytes=VMEM_BYTES),
        name="pipeline",
    )(embeds, targets, w_qkv, w_out, w_up, w_down)


def finish_kernel(num, first_unit, *refs):
    left_refs, right_refs, acc_refs, dx, out_refs, d_embeds = (
        refs[:num], refs[num : 2 * num], refs[2 * num : 3 * num], refs[3 * num], refs[3 * num + 1 : 4 * num + 1], refs[4 * num + 1])
    lefts, rights, tiles, flat, l_sem, r_sem, a_sem, o_sem, in_sem, put_sem = refs[4 * num + 2 :]
    work = WeightTiles(
        left_refs, right_refs, acc_refs, out_refs, lefts, rights, tiles, l_sem, r_sem, a_sem, o_sem, first_unit, 0)
    units = dx.shape[0]

    def fetch(unit):
        slot = lax.rem(unit, 2)
        return pltpu.make_async_copy(dx.at[unit], flat.at[slot], in_sem.at[slot])

    def wait_put(slot):
        pltpu.make_async_copy(flat.at[slot], flat.at[slot], put_sem.at[slot]).wait()

    def relayout(i):
        @pl.when(i < units)
        def _():
            @pl.when(i >= 2)
            def _():
                wait_put(lax.rem(i, 2))

            fetch(i).start()

        @pl.when((i >= 1) & (i <= units))
        def _():
            unit, slot = i - 1, lax.rem(i - 1, 2)
            fetch(unit).wait()
            for j in range(dx.shape[1]):
                pltpu.make_async_copy(
                    flat.at[slot, j], d_embeds.at[unit, :, pl.ds(j * LANE, LANE)], put_sem.at[slot]).start()

    def body(i, carry):
        relayout(i)
        work.step(i)
        return carry

    lax.fori_loop(0, work.steps, body, 0)
    for i in range(work.steps, units + 1):
        relayout(i)
    for slot in range(2):
        wait_put(slot)
    for tile in range(work.slots):
        work.wait_store(tile)


def finish(lefts, rights, sums, dx):
    units, blocks, height, _ = dx.shape
    halves = height // LANE
    first_unit = units // GROUP * GROUP
    rest = units - first_unit
    num = len(lefts)
    hbm = pl.BlockSpec(memory_space=pl.ANY)
    dma = pltpu.SemaphoreType.DMA
    return pl.pallas_call(
        functools.partial(finish_kernel, num, first_unit),
        out_shape=[jax.ShapeDtypeStruct(s.shape, F32) for s in sums] + [jax.ShapeDtypeStruct((units, height, blocks * LANE), BF16)],
        in_specs=[hbm] * (3 * num + 1),
        out_specs=[hbm] * (num + 1),
        scratch_shapes=[
            pltpu.VMEM((2, rest, halves, TILE_M, LANE), BF16), pltpu.VMEM((2, rest, TILE_N // LANE, height, LANE), BF16),
            pltpu.VMEM((4, TILE_M, TILE_N), F32), pltpu.VMEM((2, blocks, height, LANE), BF16),
            dma((2,)), dma((2,)), dma((4,)), dma((4,)), dma((2,)), dma((2,))],
        compiler_params=pltpu.CompilerParams(vmem_limit_bytes=VMEM_BYTES),
        name="finish",
    )(*lefts, *rights, *sums, dx)


def solution(mesh):
    num_stages = mesh.shape["stage"]

    def stage_program(embeds, targets, w_qkv, w_out, w_up, w_down):
        num_micro, batch_size, seq_len, model_dim = embeds.shape
        num_heads, head_dim = w_out.shape[1], w_out.shape[2]
        flat = (num_micro * batch_size, seq_len, model_dim)
        res = run_pipeline(
            "stage", num_stages, embeds.reshape(flat), targets.reshape(flat),
            w_qkv[0], w_out[0].reshape(num_heads * head_dim, model_dim), w_up[0], w_down[0], head_dim)
        d_qkv, d_out, d_up, d_down, d_embeds = finish(res[:4], res[4:8], res[9:13], res[8])
        total = jnp.sum(res[-1]).reshape(1)
        return total, d_qkv[None], d_out.reshape(w_out.shape), d_up[None], d_down[None], d_embeds.reshape(embeds.shape)

    act_spec = P("rep", None, None, None)
    w3_spec = P("stage", None, None)
    g3_spec = P(("rep", "stage"), None, None)
    in_specs = (act_spec, act_spec, w3_spec, P("stage", None, None, None), w3_spec, w3_spec)
    out_specs = (P("rep"), g3_spec, P(("rep", "stage"), None, None, None), g3_spec, g3_spec, act_spec)
    return jax.shard_map(stage_program, mesh=mesh, in_specs=in_specs, out_specs=out_specs, check_vma=False)
```

```python
import functools

import jax
import jax.numpy as jnp
from jax import lax
from jax.experimental import pallas as pl
from jax.experimental.pallas import tpu as pltpu
from jax.sharding import PartitionSpec as P


F32, BF16 = jnp.float32, jnp.bfloat16
MESH = pl.DeviceIdType.MESH
NORM_EPS = 1e-6
NEG_BIG = -1e30
GELU_SCALE, GELU_CUBE = 0.7978845608028654, 0.044715
LANE = 128
NORM_ROWS = 32
RING = 3
TILE_M, TILE_N = 1024, 512
GROUP, GROUPS = 7, 1
SPLIT_UNITS = 5
TILES_BETWEEN, TILES_AFTER = 3, 8
VMEM_BYTES = 67043328


def mm(lhs, rhs):
    return jnp.dot(lhs, rhs, preferred_element_type=F32)


def mm_rt(lhs, rhs):
    return lax.dot_general(lhs, rhs, (((1,), (1,)), ((), ())), preferred_element_type=F32)


def mm_lt(lhs, rhs):
    return lax.dot_general(lhs, rhs, (((0,), (0,)), ((), ())), preferred_element_type=F32)


def cols(ref, lo, hi):
    return jnp.concatenate([ref[j] for j in range(lo, hi)], 1)


def rows_of(ref, lo, hi):
    return jnp.concatenate([ref[j, lo:hi, :] for j in range(ref.shape[0])], 1)


def pieces(vals):
    return [vals[:, LANE * j : LANE * j + LANE] for j in range(vals.shape[1] // LANE)]


def put(ref, lo, vals):
    for j, piece in enumerate(pieces(vals)):
        ref[lo + j] = piece


def accumulate(ref, vals, first):
    for j, piece in enumerate(pieces(vals)):
        ref[j] = piece if first else ref[j] + piece


def row_scale(sums, width):
    return jnp.sum(sums, axis=-1, keepdims=True) * (1.0 / width)


def norm_into(dst, load, starts):
    blocks = dst.shape[0]
    for r in starts:
        vals = [load(j, r) for j in range(blocks)]
        total = sum(v * v for v in vals)
        scale = lax.rsqrt(row_scale(total, blocks * LANE) + NORM_EPS)
        for j, v in enumerate(vals):
            dst[j, r : r + NORM_ROWS, :] = (v * scale).astype(BF16)


def norm_vjp_into(dst, base, load, d_load):
    blocks, height = dst.shape[0], dst.shape[1]
    width = blocks * LANE
    for r in range(0, height, NORM_ROWS):
        vals = [load(j, r) for j in range(blocks)]
        grads = [d_load(j, r) for j in range(blocks)]
        scale = lax.rsqrt(row_scale(sum(v * v for v in vals), width) + NORM_EPS)
        pull = scale * scale * scale * row_scale(sum(v * d for v, d in zip(vals, grads)), width)
        for j in range(blocks):
            dst[j, r : r + NORM_ROWS, :] = (base(j, r) + (grads[j] * scale - vals[j] * pull)).astype(BF16)


def reader(ref):
    return lambda j, r: ref[j, r : r + NORM_ROWS, :].astype(F32)


def rounded(ref):
    return lambda j, r: ref[j, r : r + NORM_ROWS, :].astype(BF16).astype(F32)


def gelu(x):
    t = jnp.tanh(x * (GELU_SCALE + (GELU_SCALE * GELU_CUBE) * (x * x)))
    return (0.5 * x) * (1.0 + t)


def gelu_grad(x):
    x_sq = x * x
    t = jnp.tanh(x * (GELU_SCALE + (GELU_SCALE * GELU_CUBE) * x_sq))
    up = 1.0 + t
    return 0.5 * (up + (((1.0 - t) * up) * x) * (GELU_SCALE + (3 * GELU_SCALE * GELU_CUBE) * x_sq))


def head_half(vals, which):
    lane = lax.broadcasted_iota(jnp.int32, (1, LANE), 1)
    return jnp.where((lane < LANE // 2) if which == 0 else (lane >= LANE // 2), vals, jnp.zeros_like(vals))


def split_heads(vals):
    return [head_half(vals, 0), head_half(vals, 1)]


def pair_scores(keys, queries, halves=(0, 1)):
    return [mm_rt(keys[: LANE * (t + 1)], queries[LANE * t : LANE * (t + 1)]) for t in halves]


def column_softmax(scores):
    e = jnp.exp(scores - jnp.max(scores, axis=0, keepdims=True))
    return e * (1.0 / jnp.sum(e, axis=0, keepdims=True))


def probs(scores, causal, scale, halves=(0, 1)):
    parts = []
    for t, s in zip(halves, scores):
        s = (s * scale).astype(BF16).astype(F32)
        below = jnp.where(causal, s[LANE * t :], NEG_BIG)
        parts.append(column_softmax(jnp.concatenate([s[: LANE * t], below], 0) if t else below))
    return parts


def causal_mask():
    return lax.broadcasted_iota(jnp.int32, (LANE, LANE), 0) <= lax.broadcasted_iota(jnp.int32, (LANE, LANE), 1)


def skip():
    pass


def layer_forward(halves, x, w_qkv, w_out, w_up, w_down, u, qkv, ctx_t, hid, pre, gl, out, acc, u_t, z_t, gl_t, scale, marks):
    blocks = x.shape[0]
    ff_blocks = w_up.shape[0]
    quads = blocks // 2
    half = LANE // 2
    causal = causal_mask()
    rows = slice(LANE * halves[0], LANE * (halves[-1] + 1))
    starts = range(rows.start, rows.stop, NORM_ROWS)
    norm_into(u, reader(x), starts)

    def lhs(ref, lo, hi):
        return jnp.concatenate([ref[j, rows, :] for j in range(lo, hi)], 1)

    def store(ref, lo, vals):
        for j, piece in enumerate(pieces(vals)):
            ref[lo + j, rows, :] = piece

    def gather(vals, first):
        for j, piece in enumerate(pieces(vals)):
            acc[j, rows, :] = piece if first else acc[j, rows, :] + piece

    def flip(dsts, src, lo, hi):
        per = dsts[0].shape[1] // LANE
        for j in range(lo, hi):
            at = slice(LANE * (j % per), LANE * (j % per) + LANE)
            for t, piece in zip(halves, pieces(src[j, rows, :].T)):
                dsts[j // per][t, at, :] = piece

    def project(i):
        for w in range(3):
            lo = w * blocks + 2 * i
            store(qkv, lo, mm(lhs(u, 0, blocks), cols(w_qkv, lo, lo + 2)).astype(BF16))

    def out_part(lo, hi):
        return mm_lt(jnp.concatenate([ctx_t[t, lo:hi, :] for t in halves], 1), rows_of(w_out, lo, hi))

    project(0)
    flip([u_t], u, 0, blocks)
    for i in range(quads):
        pairs = (2 * i, 2 * i + 1)
        scores = [pair_scores(k, qkv[p], halves) for p in pairs for k in split_heads(qkv[blocks + p])]
        if i < quads - 1:
            project(i + 1)
        else:
            marks.get("qkv", skip)()
            gather(out_part(0, 2 * LANE * i), True)
        a = [probs(s, causal, scale, halves) for s in scores]
        for j, p in enumerate(pairs):
            v_t = qkv[2 * blocks + p].T
            for h in range(2):
                at = slice(LANE * p + half * h, LANE * p + half * h + half)
                v_head = v_t[half * h : half * h + half]
                for t, a_part in zip(halves, a[2 * j + h]):
                    ctx_t[t, at, :] = mm(v_head[:, : LANE * (t + 1)], a_part.astype(BF16)).astype(BF16)
    gather(out_part(2 * LANE * (quads - 1), blocks * LANE), False)
    marks.get("ctx", skip)()
    for r in starts:
        for j in range(blocks):
            at = slice(r, r + NORM_ROWS)
            hid[j, at, :] = (x[j, at, :].astype(F32) + acc[j, at, :]).astype(BF16)
    norm_into(u, reader(hid), starts)
    step = 4
    up = lambda c: mm(lhs(u, 0, blocks), cols(w_up, c, c + step)).astype(BF16)
    cur = up(0)
    flip([z_t], u, 0, blocks)
    for c in range(0, ff_blocks, step):
        nxt = up(c + step) if c + step < ff_blocks else None
        for j, piece in enumerate(pieces(cur)):
            pre[c + j, rows, :] = piece
            gl[c + j, rows, :] = gelu(piece.astype(F32)).astype(BF16)
        flip(gl_t, gl, c, c + step)
        cur = nxt
    marks.get("ff", skip)()
    for j, piece in enumerate(pieces(mm(lhs(gl, 0, ff_blocks), cols(w_down, 0, blocks)))):
        out[j, rows, :] = (hid[j, rows, :].astype(F32) + piece).astype(BF16)


def layer_backward(g, x, hid, qkv, pre, w_qkv, w_out, w_up, w_down, d_qkv, d_ctx, d_hid, d_pre, out, acc, scale, marks):
    blocks = x.shape[0]
    ff_blocks = w_up.shape[0]
    quads = blocks // 2
    half = LANE // 2
    causal = causal_mask()
    step = 4
    down = lambda c: mm_rt(cols(g, 0, blocks), rows_of(w_down, LANE * c, LANE * (c + step))).astype(BF16)
    cur = down(0)
    for c in range(0, ff_blocks, step):
        nxt = down(c + step) if c + step < ff_blocks else None
        for j, piece in enumerate(pieces(cur)):
            d_pre[c + j] = (piece.astype(F32) * gelu_grad(pre[c + j].astype(F32))).astype(BF16)
        accumulate(acc, mm_rt(cols(d_pre, c, c + step), cols(w_up, c, c + step)), c == 0)
        cur = nxt
    norm_vjp_into(d_hid, reader(g), reader(hid), rounded(acc))
    marks["ff"]()

    def ctx_part(i):
        put(d_ctx, 2 * i, mm_rt(cols(d_hid, 0, blocks), rows_of(w_out, 2 * LANE * i, 2 * LANE * (i + 1))).astype(BF16))

    def qkv_part(i):
        take = lambda ref: jnp.concatenate([ref[w * blocks + 2 * i + t] for w in range(3) for t in range(2)], 1)
        accumulate(acc, mm_rt(take(d_qkv), take(w_qkv)), i == 0)

    ctx_part(0)
    for i in range(quads):
        pairs = (2 * i, 2 * i + 1)
        scores = [pair_scores(k, qkv[p]) for p in pairs for k in split_heads(qkv[blocks + p])]
        d_probs = [pair_scores(v, d_ctx[p]) for p in pairs for v in split_heads(qkv[2 * blocks + p])]
        if i < quads - 1:
            ctx_part(i + 1)
        if i > 0:
            qkv_part(i - 1)
        a, ds = [], []
        for s, dp in zip(scores, d_probs):
            a_pair = probs(s, causal, scale)
            dp = [d.astype(BF16).astype(F32) for d in dp]
            ds.append([(p * (d - jnp.sum(p * d, axis=0, keepdims=True))).astype(BF16) for p, d in zip(a_pair, dp)])
            a.append([p.astype(BF16) for p in a_pair])
        for j, p in enumerate(pairs):
            n = LANE

            def weigh(first, second, vals):
                top = mm(
                    jnp.concatenate([first[0], first[1][:n], second[0], second[1][:n]], 1), jnp.concatenate(vals, 0))
                low = mm(
                    jnp.concatenate([first[1][n:], second[1][n:]], 1), jnp.concatenate([vals[0][n:], vals[1][n:]], 0))
                return jnp.concatenate([top, low], 0)

            heads = (2 * j, 2 * j + 1)
            d_qkv[2 * blocks + p] = weigh(*(a[h] for h in heads), split_heads(d_ctx[p])).astype(BF16)
            d_qkv[blocks + p] = (weigh(*(ds[h] for h in heads), split_heads(qkv[p])) * scale).astype(BF16)
            k_t = qkv[blocks + p].T
            dq_t = []
            for h in range(2):
                k_head = k_t[half * h : half * h + half]
                d0, d1 = ds[heads[h]]
                dq_t.append(jnp.concatenate([mm(k_head[:, :n], d0), mm(k_head, d1)], 1) * scale)
            d_qkv[p] = jnp.concatenate(dq_t, 0).astype(BF16).T
    qkv_part(quads - 1)
    marks["qkv"]()
    norm_vjp_into(out, reader(d_hid), reader(x), rounded(acc))


class WeightTiles:
    def __init__(self, left_refs, right_refs, acc_refs, out_refs, lefts, rights, tiles, l_sem, r_sem, a_sem, o_sem, first_unit, bare):
        self.left_refs, self.right_refs, self.acc_refs, self.out_refs = left_refs, right_refs, acc_refs, out_refs
        self.lefts, self.rights, self.tiles = lefts, rights, tiles
        self.l_sem, self.r_sem, self.a_sem, self.o_sem = l_sem, r_sem, a_sem, o_sem
        self.first_unit = first_unit
        self.units, self.halves = lefts.shape[1], lefts.shape[2]
        self.slots, self.ahead = tiles.shape[0], rights.shape[0] - 1
        self.sums = bare == 0
        self.spans, self.steps = [], 0
        for w, (a, b) in enumerate(zip(left_refs, right_refs)):
            count = b.shape[1] * LANE // TILE_N
            for m in range(a.shape[2] // TILE_M):
                self.spans.append((w, m, self.steps, count))
                self.steps += count

    def group_units(self, group):
        return pl.ds(self.first_unit + group * self.units, self.units)

    def left_copy(self, k, group):
        w, m = self.spans[k][:2]
        src = self.left_refs[w].at[self.group_units(group), :, pl.ds(m * TILE_M, TILE_M), :]
        return pltpu.make_async_copy(src, self.lefts.at[k % 2], self.l_sem.at[k % 2])

    def each_span(self, j, fn):
        for w, m, first, count in self.spans:
            @pl.when((j >= first) & (j < first + count))
            def _():
                fn(w, m, j - first)

    def window(self, refs, w, m, n):
        return refs[w].at[pl.ds(m * TILE_M, TILE_M), pl.ds(pl.multiple_of(n * TILE_N, TILE_N), TILE_N)]

    def load(self, i):
        group, j = i // self.steps, lax.rem(i, self.steps)
        slot, tile = lax.rem(i, self.ahead + 1), lax.rem(i, self.slots)
        per = TILE_N // LANE

        @pl.when(i >= self.slots)
        def _():
            if self.sums:
                self.wait_store(tile)

        def start(w, m, n):
            src = self.right_refs[w].at[self.group_units(group), pl.ds(n * per, per)]
            pltpu.make_async_copy(src, self.rights.at[slot], self.r_sem.at[slot]).start()

            if self.sums:
                pltpu.make_async_copy(
                    self.window(self.acc_refs, w, m, n), self.tiles.at[tile], self.a_sem.at[tile]).start()

        self.each_span(j, start)

    def wait_store(self, tile):
        pltpu.make_async_copy(self.tiles.at[tile], self.tiles.at[tile], self.o_sem.at[tile]).wait()

    def step(self, i):
        group, j = i // self.steps, lax.rem(i, self.steps)
        slot, tile = lax.rem(i, self.ahead + 1), lax.rem(i, self.slots)

        @pl.when(j == 0)
        def _():
            self.left_copy(0, group).start()
            for d in range(self.ahead):
                self.load(i + d)
            self.left_copy(1, group).start()

        @pl.when(j + self.ahead < self.steps)
        def _():
            self.load(i + self.ahead)

        chunk = -1
        for k, (_, _, first, _) in enumerate(self.spans):
            chunk = chunk + jnp.where(j >= first, 1, 0)

            @pl.when(j == first)
            def _():
                self.left_copy(k, group).wait()
                if 0 < k < len(self.spans) - 1:
                    self.left_copy(k + 1, group).start()

        pltpu.make_async_copy(self.rights.at[slot], self.rights.at[slot], self.r_sem.at[slot]).wait()

        if self.sums:
            pltpu.make_async_copy(self.tiles.at[tile], self.tiles.at[tile], self.a_sem.at[tile]).wait()
        else:
            @pl.when(i >= self.slots)
            def _():
                self.wait_store(tile)

        a_ref, b_ref = self.lefts.at[lax.rem(chunk, 2)], self.rights.at[slot]
        a = jnp.concatenate([a_ref[k, t] for k in range(self.units) for t in range(self.halves)], 1)
        b = jnp.concatenate([cols(b_ref.at[k], 0, TILE_N // LANE) for k in range(self.units)], 0)
        fresh = mm(a, b)
        self.tiles[tile] = self.tiles[tile] + fresh if self.sums else fresh

        def store(w, m, n):
            pltpu.make_async_copy(self.tiles.at[tile], self.window(self.out_refs, w, m, n), self.o_sem.at[tile]).start()

        self.each_span(j, store)


def pipeline_kernel(
    axis, stages, units, scale, inv_count,
    embeds, targets, w_qkv_h, w_out_h, w_up_h, w_down_h,
    ut_all, ctx_all, zt_all, glt_all, dqkv_all, dh_all, dpre_all, g_all, dx_all,
    gw_qkv, gw_out, gw_up, gw_down, qkv_all, h_all, pre_all, x_all, loss,
    w_qkv, w_out, w_up, w_down, act, grad, out, d_in,
    tmp_act, tmp_mid, tmp_ff, qkv, hid, pre, acc, dqkv, lefts, rights, tiles,
    w_sem, emb_sem, tgt_sem, f_send, f_recv, f_free, b_send, b_recv, b_free, f_save, b_save, b_load,
    x_send, x_recv, l_send, l_recv, wl_sem, wr_sem, wa_sem, wo_sem,
):
    stage = lax.axis_index(axis)
    last = stages - 1
    blocks, height = act.shape[1], act.shape[2]
    halves = range(height // LANE)
    right, left = lax.rem(stage + 1, stages), lax.rem(stage + last, stages)
    u = dctx = tmp_act
    target = dh = tmp_mid
    gl = dpre = tmp_ff
    chunks = w_down.shape[1] // TILE_M
    gl_t = [lefts.at[0, k] for k in range(chunks)]
    u_t, z_t, ctx_t = lefts.at[0, chunks], lefts.at[0, chunks + 1], lefts.at[1, 0]
    gw = (gw_qkv, gw_out, gw_up, gw_down)
    work = WeightTiles(
        (ut_all, ctx_all, zt_all, glt_all), (dqkv_all, dh_all, dpre_all, g_all), gw, gw, lefts, rights, tiles,
        wl_sem, wr_sem, wa_sem, wo_sem, 0, 1)
    total_tiles = GROUPS * work.steps
    barrier = pltpu.get_barrier_semaphore()
    for ahead in range(1, stages):
        pl.semaphore_signal(
            barrier, inc=1, device_id={axis: lax.rem(stage + ahead, stages)}, device_id_type=MESH)

    def load_columns(src, dst, sem):
        def start(j, carry):
            pltpu.make_async_copy(src.at[:, pl.ds(pl.multiple_of(j * LANE, LANE), LANE)], dst.at[j], sem).start()
            return carry

        lax.fori_loop(0, dst.shape[0], start, 0)

    def wait_whole(ref, sem):
        pltpu.make_async_copy(ref, ref, sem).wait()

    def embed_slot(unit):
        return act.at[lax.rem(unit, RING)], emb_sem.at[lax.rem(unit, RING)]

    def embed_start(unit):
        load_columns(embeds.at[unit], *embed_slot(unit))

    weights = ((w_qkv_h, w_qkv), (w_out_h, w_out), (w_up_h, w_up), (w_down_h, w_down))

    @pl.when(stage == 0)
    def _():
        embed_start(0)

    for i, (src, dst) in enumerate(weights):
        load_columns(src, dst, w_sem.at[i])

    @pl.when(stage == 0)
    def _():
        embed_start(1)

    loss[...] = jnp.zeros_like(loss)
    pl.semaphore_wait(barrier, last)

    def f_copy(unit, half):
        slot, ring = lax.rem(unit, 2), lax.rem(unit, RING)
        at = pl.ds(half * LANE, LANE)
        return pltpu.make_async_remote_copy(
            src_ref=out.at[slot, :, at, :], dst_ref=act.at[ring, :, at, :], send_sem=f_send.at[slot, half],
            recv_sem=f_recv.at[ring, half], device_id={axis: right}, device_id_type=MESH)

    def b_copy(unit):
        slot, ring = lax.rem(unit, 2), lax.rem(unit, RING)
        return pltpu.make_async_remote_copy(
            src_ref=d_in.at[slot], dst_ref=grad.at[ring], send_sem=b_send.at[slot], recv_sem=b_recv.at[ring],
            device_id={axis: left}, device_id_type=MESH)

    even = lax.rem(stage, 2) == 0
    chain = even & ((stage == 0) | (stage + 2 < stages - 2))
    branches = ((even, right), (chain, lax.rem(stage + 2, stages)), (stage == 0, stages - 2))

    def x_copies(unit, src):
        slot = lax.rem(unit, 2)
        return [
            (cond, pltpu.make_async_remote_copy(
                src_ref=src, dst_ref=dx_all.at[unit], send_sem=x_send.at[slot, k], recv_sem=x_recv.at[unit],
                device_id={axis: dest}, device_id_type=MESH))
            for k, (cond, dest) in enumerate(branches)]

    def x_start(unit, src):
        for cond, copy in x_copies(unit, src):
            @pl.when(cond)
            def _():
                copy.start()

    def x_wait_send(unit):
        for cond, copy in x_copies(unit, dx_all.at[unit]):
            @pl.when(cond)
            def _():
                copy.wait_send()

    def x_wait_recv(unit):
        x_copies(unit, dx_all.at[unit])[0][1].wait_recv()

    def dx_copy(unit):
        slot = lax.rem(unit, 2)
        return pltpu.make_async_copy(d_in.at[slot], dx_all.at[unit], b_send.at[slot])

    def loss_copy(k):
        return pltpu.make_async_remote_copy(
            src_ref=loss, dst_ref=loss, send_sem=l_send.at[k], recv_sem=l_recv, device_id={axis: k}, device_id_type=MESH)

    def f_saves(unit):
        pairs = [
            (act.at[lax.rem(unit, RING)], x_all.at[unit]), (u_t, ut_all.at[unit]), (qkv.at[0], qkv_all.at[unit]),
            (ctx_t, ctx_all.at[unit]), (hid.at[0], h_all.at[unit]), (z_t, zt_all.at[unit]), (pre.at[0], pre_all.at[unit])]
        pairs += [(ref, glt_all.at[unit, :, pl.ds(k * TILE_M, TILE_M), :]) for k, ref in enumerate(gl_t)]
        return [pltpu.make_async_copy(src, dst, f_save.at[i]) for i, (src, dst) in enumerate(pairs)]

    def b_saves(unit):
        pairs = ((grad.at[lax.rem(unit, RING)], g_all), (dqkv, dqkv_all), (dpre, dpre_all), (dh, dh_all))
        return [pltpu.make_async_copy(src, dst.at[unit], b_save.at[i]) for i, (src, dst) in enumerate(pairs)]

    def b_loads(unit):
        pairs = (
            (pre_all, pre.at[1]), (h_all, hid.at[1]), (qkv_all, qkv.at[1]), (x_all, act.at[RING + lax.rem(unit, 2)]))
        return [pltpu.make_async_copy(src.at[unit], dst, b_load.at[i]) for i, (src, dst) in enumerate(pairs)]

    def wait_late_saves(unit):
        for copy in b_saves(unit)[:2]:
            copy.wait()

    work_start = jnp.maximum(GROUP - 1 + 2 * last - stage, units + stage)
    b_end = units - 1 + 2 * last - stage

    def tiles_by(t):
        between = jnp.maximum(jnp.minimum(t, b_end) - work_start + 1, 0)
        return jnp.minimum(TILES_BETWEEN * between + TILES_AFTER * jnp.maximum(t - b_end, 0), total_tiles)

    def make_tiles(first, end):
        lax.fori_loop(first, end, lambda i, c: (work.step(i), c)[1], 0)

    def forward(unit):
        ring, slot = lax.rem(unit, RING), lax.rem(unit, 2)
        saves = f_saves(unit)

        @pl.when(stage == last)
        def _():
            load_columns(targets.at[unit], target, tgt_sem)

        @pl.when((stage == 0) & (unit + 2 < units))
        def _():
            embed_start(unit + 2)

        @pl.when((stage < last) & (unit >= 2))
        def _():
            for half in halves:
                f_copy(unit, half).wait_send()

        def run(part, marks):
            layer_forward(
                part, act.at[ring], w_qkv, w_out, w_up, w_down, u, qkv.at[0], ctx_t, hid.at[0], pre.at[0], gl,
                out.at[slot], acc, u_t, z_t, gl_t, scale, marks)

        def arrive(half):
            @pl.when((stage == 0) & (half == 0))
            def _():
                wait_whole(*embed_slot(unit))

            @pl.when(stage > 0)
            def _():
                f_copy(unit, half).wait_recv()

        def leave(half):
            @pl.when(stage < last)
            def _():
                f_copy(unit, half).start()

        def credit():
            @pl.when((stage < last) & (unit >= RING))
            def _():
                pl.semaphore_wait(f_free, 1)

        def weights_ready(*which):
            def wait():
                @pl.when(unit == 0)
                def _():
                    for w in which:
                        wait_whole(weights[w][1], w_sem.at[w])

            return wait

        @pl.when(unit < SPLIT_UNITS)
        def _():
            arrive(0)
            weights_ready(0)()
            run((0,), {"qkv": weights_ready(1), "ctx": weights_ready(2), "ff": weights_ready(3)})
            credit()
            leave(0)
            arrive(1)
            run((1,), {})
            leave(1)

        @pl.when(unit >= SPLIT_UNITS)
        def _():
            arrive(0)
            arrive(1)
            run((0, 1), {})
            credit()
            leave(0)
            leave(1)

        for copy in saves:
            copy.start()

        @pl.when(stage == last)
        def _():
            wait_whole(target, tgt_sem)
            part = jnp.zeros((8, LANE), F32)
            for j in range(blocks):
                err = out[slot, j].astype(F32) - target[j].astype(F32)
                grad[ring, j] = (err * inv_count).astype(BF16)
                part += jnp.sum((err * err).reshape(height // 8, 8, LANE), axis=0)
            loss[...] += part * (0.5 * inv_count)

        @pl.when((stage == last) & (unit == units - 1))
        def _():
            for k in range(stages - 1):
                loss_copy(k).start()

    def backward(unit, saved):
        ring, slot = lax.rem(unit, RING), lax.rem(unit, 2)
        src = jnp.where(stage == last, 0, 1)
        x_slot = jnp.where(stage == last, ring, RING + slot)
        saves = b_saves(unit)
        following = b_loads(unit + 1)
        more = (stage < last) & (unit + 1 < units)

        @pl.when(unit > 0)
        def _():
            @pl.when(jnp.logical_not(saved))
            def _():
                wait_late_saves(unit - 1)

            @pl.when((stage < last) & (unit - 1 < units - RING))
            def _():
                pl.semaphore_signal(b_free, inc=1, device_id={axis: right}, device_id_type=MESH)

        @pl.when(unit >= 2)
        def _():
            @pl.when(stage > 0)
            def _():
                b_copy(unit).wait_send()

            @pl.when(stage == 0)
            def _():
                dx_copy(unit).wait()
                x_wait_send(unit)

        @pl.when(stage < last)
        def _():
            b_copy(unit).wait_recv()
            for copy in b_loads(unit):
                copy.wait()

        saves[0].start()

        def ff_ready():
            saves[2].start()
            saves[3].start()

            @pl.when(more)
            def _():
                for i in (0, 1, 3):
                    following[i].start()

        def qkv_ready():
            saves[1].start()

            @pl.when(more)
            def _():
                following[2].start()

        layer_backward(
            grad.at[ring], act.at[x_slot], hid.at[src], qkv.at[src], pre.at[src], w_qkv, w_out, w_up, w_down,
            dqkv, dctx, dh, dpre, d_in.at[slot], acc, scale, {"ff": ff_ready, "qkv": qkv_ready})

        @pl.when((stage > 0) & (unit >= RING))
        def _():
            pl.semaphore_wait(b_free, 1)

        @pl.when(stage > 0)
        def _():
            b_copy(unit).start()

        @pl.when(stage == 0)
        def _():
            dx_copy(unit).start()
            x_start(unit, d_in.at[slot])

        saves[2].wait()
        saves[3].wait()

    def tick(t, carry):
        f_unit = t - stage
        b_unit = t - 2 * last + stage
        before, first, end = tiles_by(t - 2), tiles_by(t - 1), tiles_by(t)

        @pl.when((f_unit >= 1) & (f_unit <= units))
        def _():
            for copy in f_saves(f_unit - 1):
                copy.wait()

            @pl.when((stage > 0) & (f_unit - 1 < units - RING))
            def _():
                pl.semaphore_signal(f_free, inc=1, device_id={axis: left}, device_id_type=MESH)

        @pl.when((stage < last) & (b_unit == 0))
        def _():
            for copy in b_loads(0):
                copy.start()

        @pl.when((f_unit >= 0) & (f_unit < units))
        def _():
            forward(f_unit)

        @pl.when((b_unit >= 0) & (b_unit < units))
        def _():
            backward(b_unit, first > before)

            @pl.when(end > first)
            def _():
                wait_late_saves(b_unit)

        make_tiles(first, end)
        x_unit = t - 2 * last

        @pl.when(even & (stage > 0) & (x_unit >= 0))
        def _():
            x_wait_recv(x_unit)

            @pl.when(x_unit >= 2)
            def _():
                x_wait_send(x_unit)

            x_start(x_unit, dx_all.at[x_unit])

        return carry

    ticks = units + 2 * last
    lax.fori_loop(0, ticks, tick, 0)

    @pl.when(tiles_by(b_end) == tiles_by(b_end - 1))
    def _():
        wait_late_saves(units - 1)

    make_tiles(tiles_by(ticks - 1), total_tiles)

    for tile in range(work.slots):
        work.wait_store(tile)

    for unit in (units - 2, units - 1):
        @pl.when(stage < last)
        def _():
            for half in halves:
                f_copy(unit, half).wait_send()

        @pl.when(stage > 0)
        def _():
            b_copy(unit).wait_send()

        @pl.when(stage == 0)
        def _():
            dx_copy(unit).wait()

        x_wait_send(unit)

    @pl.when(jnp.logical_not(even))
    def _():
        lax.fori_loop(0, units, lambda unit, c: (x_wait_recv(unit), c)[1], 0)

    @pl.when(stage < last)
    def _():
        loss_copy(0).wait_recv()

    @pl.when(stage == last)
    def _():
        for k in range(stages - 1):
            loss_copy(k).wait_send()


def run_pipeline(axis, stages, embeds, targets, w_qkv, w_out, w_up, w_down, head_dim):
    units, height, width = embeds.shape
    n, ff = width // LANE, w_up.shape[1] // LANE
    halves = height // LANE
    saved = lambda *shape: jax.ShapeDtypeStruct((units,) + shape, BF16)
    rows_t = lambda k: saved(k, height, LANE)
    cols_t = lambda k: saved(halves, k, LANE)
    hbm = pl.BlockSpec(memory_space=pl.ANY)
    vm = lambda *shape: pltpu.VMEM(shape, BF16)
    rows = lambda *lead: vm(*lead, height, LANE)
    dma, regular = pltpu.SemaphoreType.DMA, pltpu.SemaphoreType.REGULAR
    outs = [
        cols_t(width), cols_t(width), cols_t(width), cols_t(ff * LANE), rows_t(3 * n), rows_t(n), rows_t(ff), rows_t(n), rows_t(n)]
    outs += [jax.ShapeDtypeStruct(w.shape, F32) for w in (w_qkv, w_out, w_up, w_down)]
    outs += [rows_t(3 * n), rows_t(n), rows_t(ff), rows_t(n), jax.ShapeDtypeStruct((8, LANE), F32)]
    return pl.pallas_call(
        functools.partial(pipeline_kernel, axis, stages, units, head_dim ** -0.5, 1.0 / (units * height * width)),
        out_shape=outs,
        in_specs=[hbm] * 6,
        out_specs=[hbm] * 17 + [pl.BlockSpec(memory_space=pltpu.VMEM)],
        scratch_shapes=[
            vm(3 * n, width, LANE), vm(n, width, LANE), vm(ff, width, LANE), vm(n, ff * LANE, LANE),
            rows(RING + 2, n), rows(RING, n), rows(2, n), rows(2, n),
            rows(n), rows(n), rows(ff), rows(2, 3 * n), rows(2, n), rows(2, ff), pltpu.VMEM((n, height, LANE), F32), rows(3 * n),
            vm(2, GROUP, halves, TILE_M, LANE), rows(2, GROUP, TILE_N // LANE), pltpu.VMEM((2, TILE_M, TILE_N), F32),
            dma((4,)), dma((RING,)), dma, dma((2, halves)), dma((RING, halves)), regular,
            dma((2,)), dma((RING,)), regular, dma((7 + ff * LANE // TILE_M,)), dma((4,)), dma((4,)),
            dma((2, 3)), dma((units,)), dma((stages - 1,)), dma, dma((2,)), dma((2,)), dma((2,)), dma((2,)),
        ],
        compiler_params=pltpu.CompilerParams(collective_id=0, has_side_effects=True, vmem_limit_bytes=VMEM_BYTES),
        name="pipeline",
    )(embeds, targets, w_qkv, w_out, w_up, w_down)


def finish_kernel(num, first_unit, *refs):
    left_refs, right_refs, acc_refs, dx, out_refs, d_embeds = (
        refs[:num], refs[num : 2 * num], refs[2 * num : 3 * num], refs[3 * num], refs[3 * num + 1 : 4 * num + 1], refs[4 * num + 1])
    lefts, rights, tiles, flat, l_sem, r_sem, a_sem, o_sem, in_sem, put_sem = refs[4 * num + 2 :]
    work = WeightTiles(
        left_refs, right_refs, acc_refs, out_refs, lefts, rights, tiles, l_sem, r_sem, a_sem, o_sem, first_unit, 0)
    units = dx.shape[0]

    def fetch(unit):
        slot = lax.rem(unit, 2)
        return pltpu.make_async_copy(dx.at[unit], flat.at[slot], in_sem.at[slot])

    def wait_put(slot):
        pltpu.make_async_copy(flat.at[slot], flat.at[slot], put_sem.at[slot]).wait()

    def relayout(i):
        @pl.when(i < units)
        def _():
            @pl.when(i >= 2)
            def _():
                wait_put(lax.rem(i, 2))

            fetch(i).start()

        @pl.when((i >= 1) & (i <= units))
        def _():
            unit, slot = i - 1, lax.rem(i - 1, 2)
            fetch(unit).wait()
            for j in range(dx.shape[1]):
                pltpu.make_async_copy(
                    flat.at[slot, j], d_embeds.at[unit, :, pl.ds(j * LANE, LANE)], put_sem.at[slot]).start()

    def body(i, carry):
        relayout(i)
        work.step(i)
        return carry

    lax.fori_loop(0, work.steps, body, 0)
    for i in range(work.steps, units + 1):
        relayout(i)
    for slot in range(2):
        wait_put(slot)
    for tile in range(work.slots):
        work.wait_store(tile)


def finish(lefts, rights, sums, dx):
    units, blocks, height, _ = dx.shape
    halves = height // LANE
    first_unit = GROUPS * GROUP
    rest = units - first_unit
    num = len(lefts)
    hbm = pl.BlockSpec(memory_space=pl.ANY)
    dma = pltpu.SemaphoreType.DMA
    return pl.pallas_call(
        functools.partial(finish_kernel, num, first_unit),
        out_shape=[jax.ShapeDtypeStruct(s.shape, F32) for s in sums] + [jax.ShapeDtypeStruct((units, height, blocks * LANE), BF16)],
        in_specs=[hbm] * (3 * num + 1),
        out_specs=[hbm] * (num + 1),
        scratch_shapes=[
            pltpu.VMEM((2, rest, halves, TILE_M, LANE), BF16), pltpu.VMEM((3, rest, TILE_N // LANE, height, LANE), BF16),
            pltpu.VMEM((4, TILE_M, TILE_N), F32), pltpu.VMEM((2, blocks, height, LANE), BF16),
            dma((2,)), dma((3,)), dma((4,)), dma((4,)), dma((2,)), dma((2,))],
        compiler_params=pltpu.CompilerParams(vmem_limit_bytes=VMEM_BYTES),
        name="finish",
    )(*lefts, *rights, *sums, dx)


def solution(mesh):
    num_stages = mesh.shape["stage"]

    def stage_program(embeds, targets, w_qkv, w_out, w_up, w_down):
        num_micro, batch_size, seq_len, model_dim = embeds.shape
        num_heads, head_dim = w_out.shape[1], w_out.shape[2]
        flat = (num_micro * batch_size, seq_len, model_dim)
        res = run_pipeline(
            "stage", num_stages, embeds.reshape(flat), targets.reshape(flat),
            w_qkv[0], w_out[0].reshape(num_heads * head_dim, model_dim), w_up[0], w_down[0], head_dim)
        d_qkv, d_out, d_up, d_down, d_embeds = finish(res[:4], res[4:8], res[9:13], res[8])
        total = jnp.sum(res[-1]).reshape(1)
        return total, d_qkv[None], d_out.reshape(w_out.shape), d_up[None], d_down[None], d_embeds.reshape(embeds.shape)

    act_spec = P("rep", None, None, None)
    w3_spec = P("stage", None, None)
    g3_spec = P(("rep", "stage"), None, None)
    in_specs = (act_spec, act_spec, w3_spec, P("stage", None, None, None), w3_spec, w3_spec)
    out_specs = (P("rep"), g3_spec, P(("rep", "stage"), None, None, None), g3_spec, g3_spec, act_spec)
    return jax.shard_map(stage_program, mesh=mesh, in_specs=in_specs, out_specs=out_specs, check_vma=False)
```
